16 devices in a mesh: dp: 2 (over y, z), tp: 8 (over x, core).
Axes of the slice: x: 4, y: 2, z: 1, core: 2. Of those that a mesh axis runs over, the one named last changes fastest.
The devices are a block of a 4x4x8 slice.
Arguments:
- x_steps: bfloat16 [32, 128, 2048], P(None, 'dp'), parts along dimension 1
- cur_len: int32 [128], P('dp'), parts along dimension 0
- k_cache: bfloat16 [2, 128, 128, 16, 128], P(None, 'dp', None, 'tp'), parts along dimension 1
- v_cache: bfloat16 [2, 128, 128, 16, 128], P(None, 'dp', None, 'tp'), parts along dimension 1
- ln_gain: bfloat16 [2, 2048], replicated
- ln_bias: bfloat16 [2, 2048], replicated
- w_q: bfloat16 [2, 2048, 2048], P(None, None, 'tp')
- w_k: bfloat16 [2, 2048, 2048], P(None, None, 'tp')
- w_v: bfloat16 [2, 2048, 2048], P(None, None, 'tp')
- w_o: bfloat16 [2, 2048, 2048], P(None, 'tp')
- w_in: bfloat16 [2, 2048, 8192], P(None, None, 'tp')
- b_in: bfloat16 [2, 8192], P(None, 'tp')
- w_out: bfloat16 [2, 8192, 2048], P(None, 'tp')
- b_out: bfloat16 [2, 2048], replicated
Outputs:
- output 1: bfloat16 [32, 128, 2048], P(None, 'dp'), parts along dimension 1
- output 2: bfloat16 [2, 128, 128, 16, 128], P(None, 'dp', None, 'tp'), parts along dimension 1
- output 3: bfloat16 [2, 128, 128, 16, 128], P(None, 'dp', None, 'tp'), parts along dimension 1
There are 2 independent parts. The reference program is written for one: setup_inputs(seed, part) draws one part's arguments, and reference() takes and returns one part's arrays. A program takes and returns all parts, laid end to end along the dimension named above; an argument that names none is the same for every part.
All inputs are finite; a program needn't handle non-finite values.
Results may differ from the reference program's by a relative error of at most 0.0169117.
Values are sent between devices in bfloat16 or wider.
A program may use at most 768 MiB of HBM per device.

```python
import jax
import jax.numpy as jnp
from jax import lax

D_MODEL = 2048
N_HEADS = 16
HEAD_DIM = 128
ROT_DIM = 64
FF_DIM = 8192
BATCH_PART = 64
CACHE_LEN = 128
N_STEPS = 32
N_LAYERS = 2
LN_EPS = 1e-5
QUERY_GAIN = 2.5


def setup_inputs(seed: int = 0, part: int = 0) -> dict:
    base_key = jax.random.key(seed)
    shared_keys = jax.random.split(base_key, 10)
    part_keys = jax.random.split(jax.random.fold_in(base_key, part), 6)
    scale_model = D_MODEL ** -0.5
    scale_ff = FF_DIM ** -0.5
    cache_shape = (N_LAYERS, BATCH_PART, CACHE_LEN, N_HEADS, HEAD_DIM)

    def gaussian(key, shape, scale):
        return jax.random.normal(key, shape, jnp.float32) * scale

    top_len = CACHE_LEN - N_STEPS
    raw_span = jax.random.randint(part_keys[1], (BATCH_PART,), 0, top_len)
    shift_bits = jax.random.randint(part_keys[2], (BATCH_PART,), 0, 8)
    full_row = jax.random.randint(part_keys[3], (), 0, BATCH_PART)
    cur_len = 1 + jnp.right_shift(raw_span, shift_bits)
    cur_len = jnp.where(jnp.arange(BATCH_PART) == full_row, top_len, cur_len).astype(jnp.int32)
    return {
        "x_steps": gaussian(part_keys[0], (N_STEPS, BATCH_PART, D_MODEL), 1.0).astype(jnp.bfloat16),
        "cur_len": cur_len,
        "k_cache": gaussian(part_keys[4], cache_shape, 1.0).astype(jnp.bfloat16),
        "v_cache": gaussian(part_keys[5], cache_shape, 1.0).astype(jnp.bfloat16),
        "ln_gain": (1.0 + gaussian(shared_keys[0], (N_LAYERS, D_MODEL), 0.2)).astype(jnp.bfloat16),
        "ln_bias": gaussian(shared_keys[1], (N_LAYERS, D_MODEL), 0.2).astype(jnp.bfloat16),
        "w_q": gaussian(shared_keys[2], (N_LAYERS, D_MODEL, D_MODEL), QUERY_GAIN * scale_model).astype(jnp.bfloat16),
        "w_k": gaussian(shared_keys[3], (N_LAYERS, D_MODEL, D_MODEL), scale_model).astype(jnp.bfloat16),
        "w_v": gaussian(shared_keys[4], (N_LAYERS, D_MODEL, D_MODEL), scale_model).astype(jnp.bfloat16),
        "w_o": gaussian(shared_keys[5], (N_LAYERS, D_MODEL, D_MODEL), scale_model).astype(jnp.bfloat16),
        "w_in": gaussian(shared_keys[6], (N_LAYERS, D_MODEL, FF_DIM), scale_model).astype(jnp.bfloat16),
        "b_in": gaussian(shared_keys[7], (N_LAYERS, FF_DIM), 0.5).astype(jnp.bfloat16),
        "w_out": gaussian(shared_keys[8], (N_LAYERS, FF_DIM, D_MODEL), scale_ff).astype(jnp.bfloat16),
        "b_out": gaussian(shared_keys[9], (N_LAYERS, D_MODEL), 0.3).astype(jnp.bfloat16),
    }


def layer_norm(hidden, gain, bias):
    hid_f32 = hidden.astype(jnp.float32)
    row_mean = jnp.mean(hid_f32, axis=-1, keepdims=True)
    centered = hid_f32 - row_mean
    row_var = jnp.mean(centered * centered, axis=-1, keepdims=True)
    normed = centered / jnp.sqrt(row_var + LN_EPS)
    return (normed * gain.astype(jnp.float32) + bias.astype(jnp.float32)).astype(jnp.bfloat16)


def rotary_tables(positions):
    inv_freq = 1.0 / (10000.0 ** (jnp.arange(0, ROT_DIM, 2).astype(jnp.float32) / ROT_DIM))
    angles = positions.astype(jnp.float32)[:, None] * inv_freq[None, :]
    return jnp.cos(angles)[:, None, :], jnp.sin(angles)[:, None, :]


def apply_rotary(vectors, cos_tab, sin_tab):
    lead_shape = vectors.shape[:-1]
    pairs = vectors[..., :ROT_DIM].reshape(lead_shape + (ROT_DIM // 2, 2))
    even_part = pairs[..., 0]
    odd_part = pairs[..., 1]
    rotated = jnp.stack([even_part * cos_tab - odd_part * sin_tab, odd_part * cos_tab + even_part * sin_tab], axis=-1)
    return jnp.concatenate([rotated.reshape(lead_shape + (ROT_DIM,)), vectors[..., ROT_DIM:]], axis=-1)


def decoder_layer(hidden, new_pos, layer):
    (k_layer, v_layer, gain, bias, q_weight, k_weight, v_weight, o_weight,
     in_weight, in_bias, out_weight, out_bias) = layer
    batch = hidden.shape[0]
    head_shape = (batch, N_HEADS, HEAD_DIM)
    normed = layer_norm(hidden, gain, bias)
    query = jnp.dot(normed, q_weight, preferred_element_type=jnp.float32).reshape(head_shape)
    key_new = jnp.dot(normed, k_weight, preferred_element_type=jnp.float32).reshape(head_shape)
    value_new = jnp.dot(normed, v_weight, preferred_element_type=jnp.float32).reshape(head_shape).astype(jnp.bfloat16)
    cos_tab, sin_tab = rotary_tables(new_pos)
    query = apply_rotary(query, cos_tab, sin_tab).astype(jnp.bfloat16)
    key_new = apply_rotary(key_new, cos_tab, sin_tab).astype(jnp.bfloat16)
    slot_ids = jnp.arange(CACHE_LEN)
    written = (slot_ids[None, :] == new_pos[:, None])[:, :, None, None]
    k_layer = jnp.where(written, key_new[:, None], k_layer)
    v_layer = jnp.where(written, value_new[:, None], v_layer)
    scores = jnp.einsum("bhe,bshe->bhs", query.astype(jnp.float32), k_layer.astype(jnp.float32)) * (HEAD_DIM ** -0.5)
    visible = (slot_ids[None, :] <= new_pos[:, None])[:, None, :]
    scores = jnp.where(visible, scores, -jnp.inf)
    exp_scores = jnp.exp(scores - jnp.max(scores, axis=-1, keepdims=True))
    attn_probs = (exp_scores / jnp.sum(exp_scores, axis=-1, keepdims=True)).astype(jnp.bfloat16)
    context = jnp.einsum("bhs,bshe->bhe", attn_probs.astype(jnp.float32), v_layer.astype(jnp.float32))
    context = context.astype(jnp.bfloat16).reshape(batch, N_HEADS * HEAD_DIM)
    attn_out = jnp.dot(context, o_weight, preferred_element_type=jnp.float32)
    pre_act = jnp.dot(normed, in_weight, preferred_element_type=jnp.float32) + in_bias.astype(jnp.float32)
    gelu_act = jax.nn.gelu(pre_act, approximate=True).astype(jnp.bfloat16)
    mlp_out = jnp.dot(gelu_act, out_weight, preferred_element_type=jnp.float32)
    new_hidden = (hidden.astype(jnp.float32) + attn_out + mlp_out + out_bias.astype(jnp.float32)).astype(jnp.bfloat16)
    return new_hidden, (k_layer, v_layer)


def reference(x_steps, cur_len, k_cache, v_cache, ln_gain, ln_bias, w_q, w_k, w_v, w_o, w_in, b_in, w_out, b_out):
    def one_step(caches, step_in):
        x_now, step_idx = step_in
        new_pos = cur_len + step_idx

        def layer_step(hidden, layer):
            return decoder_layer(hidden, new_pos, layer)

        layers = (caches[0], caches[1], ln_gain, ln_bias, w_q, w_k, w_v, w_o, w_in, b_in, w_out, b_out)
        last_hidden, new_caches = lax.scan(layer_step, x_now, layers)
        return new_caches, last_hidden

    final_caches, hidden_out = lax.scan(one_step, (k_cache, v_cache), (x_steps, jnp.arange(N_STEPS, dtype=jnp.int32)))
    return hidden_out, final_caches[0], final_caches[1]
```

```python
import jax
import jax.numpy as jnp
from jax import lax
from jax.sharding import PartitionSpec as P

ROT_DIM = 64
LN_EPS = 1e-5
N_CHUNKS = 4


def layer_norm(hidden, gain, bias):
    hid_f32 = hidden.astype(jnp.float32)
    row_mean = jnp.mean(hid_f32, axis=-1, keepdims=True)
    centered = hid_f32 - row_mean
    row_var = jnp.mean(centered * centered, axis=-1, keepdims=True)
    normed = centered * lax.rsqrt(row_var + LN_EPS)
    return (normed * gain.astype(jnp.float32) + bias.astype(jnp.float32)).astype(jnp.bfloat16)


def rotary_tables(positions):
    inv_freq = 1.0 / (10000.0 ** (jnp.arange(0, ROT_DIM, 2).astype(jnp.float32) / ROT_DIM))
    angles = positions.astype(jnp.float32)[..., None] * inv_freq
    return jnp.cos(angles)[:, :, None, :], jnp.sin(angles)[:, :, None, :]


def apply_rotary(vectors, cos_tab, sin_tab):
    lead_shape = vectors.shape[:-1]
    pairs = vectors[..., :ROT_DIM].reshape(lead_shape + (ROT_DIM // 2, 2))
    even_part = pairs[..., 0]
    odd_part = pairs[..., 1]
    rotated = jnp.stack([even_part * cos_tab - odd_part * sin_tab, odd_part * cos_tab + even_part * sin_tab], axis=-1)
    return jnp.concatenate([rotated.reshape(lead_shape + (ROT_DIM,)), vectors[..., ROT_DIM:]], axis=-1)


def layer_chunk(hidden, positions, k_old, v_old, gain, bias, weights):
    q_weight, k_weight, v_weight, o_weight, in_weight, in_bias, out_weight = weights
    steps, batch, _ = hidden.shape
    _, slots, heads, head_dim = k_old.shape
    normed = layer_norm(hidden, gain, bias)
    head_shape = (steps, batch, heads, head_dim)
    dot = lambda a, w: jnp.einsum("tbd,df->tbf", a, w, preferred_element_type=jnp.float32)
    rotary = rotary_tables(positions)
    query = apply_rotary(dot(normed, q_weight).reshape(head_shape), *rotary).astype(jnp.bfloat16)
    key_new = apply_rotary(dot(normed, k_weight).reshape(head_shape), *rotary).astype(jnp.bfloat16)
    value_new = dot(normed, v_weight).reshape(head_shape).astype(jnp.bfloat16)
    slot_ids = jnp.arange(slots)
    place = positions.T[:, None, :] == slot_ids[None, :, None]
    written = jnp.any(place, axis=-1)[:, :, None, None]
    onehot = place.astype(jnp.bfloat16)
    put = lambda new, old: jnp.where(
        written, jnp.einsum("bst,tbhe->bshe", onehot, new, preferred_element_type=jnp.float32).astype(jnp.bfloat16), old)
    k_all = put(key_new, k_old)
    v_all = put(value_new, v_old)
    scores = jnp.einsum("tbhe,bshe->bhts", query, k_all, preferred_element_type=jnp.float32) * (head_dim ** -0.5)
    visible = slot_ids[None, None, None, :] <= positions.T[:, None, :, None]
    scores = jnp.where(visible, scores, -jnp.inf)
    exp_scores = jnp.exp(scores - jnp.max(scores, axis=-1, keepdims=True))
    probs = (exp_scores / jnp.sum(exp_scores, axis=-1, keepdims=True)).astype(jnp.bfloat16)
    context = jnp.einsum("bhts,bshe->tbhe", probs, v_all, preferred_element_type=jnp.float32).astype(jnp.bfloat16)
    context = context.reshape(steps, batch, heads * head_dim)
    pre_act = dot(normed, in_weight) + in_bias.astype(jnp.float32)
    act = jax.nn.gelu(pre_act, approximate=True).astype(jnp.bfloat16)
    return dot(context, o_weight) + dot(act, out_weight), k_all, v_all


def decode_shard(x_steps, cur_len, k_cache, v_cache, ln_gain, ln_bias, w_q, w_k, w_v, w_o, w_in, b_in, w_out, b_out):
    steps, batch, _ = x_steps.shape
    n_layers = k_cache.shape[0]
    size = batch // N_CHUNKS
    positions = cur_len[None, :] + jnp.arange(steps)[:, None]
    hidden = [x_steps[:, c * size:(c + 1) * size] for c in range(N_CHUNKS)]
    k_layers, v_layers = [], []
    for layer in range(n_layers):
        weights = (w_q[layer], w_k[layer], w_v[layer], w_o[layer], w_in[layer], b_in[layer], w_out[layer])
        k_parts, v_parts = [], []
        for c in range(N_CHUNKS):
            rows = slice(c * size, (c + 1) * size)
            part, k_new, v_new = layer_chunk(hidden[c], positions[:, rows], k_cache[layer, rows], v_cache[layer, rows],
                                             ln_gain[layer], ln_bias[layer], weights)
            total = lax.psum(part.astype(jnp.bfloat16), "tp")
            hidden[c] = (hidden[c].astype(jnp.float32) + total.astype(jnp.float32)
                         + b_out[layer].astype(jnp.float32)).astype(jnp.bfloat16)
            k_parts.append(k_new)
            v_parts.append(v_new)
        k_layers.append(jnp.concatenate(k_parts))
        v_layers.append(jnp.concatenate(v_parts))
    return jnp.concatenate(hidden, axis=1), jnp.stack(k_layers), jnp.stack(v_layers)


def solution(mesh):
    cache_spec = P(None, "dp", None, "tp", None)
    in_specs = (P(None, "dp", None), P("dp"), cache_spec, cache_spec, P(None, None), P(None, None),
                P(None, None, "tp"), P(None, None, "tp"), P(None, None, "tp"), P(None, "tp", None),
                P(None, None, "tp"), P(None, "tp"), P(None, "tp", None), P(None, None))
    out_specs = (P(None, "dp", None), cache_spec, cache_spec)
    return jax.shard_map(decode_shard, mesh=mesh, in_specs=in_specs, out_specs=out_specs, check_vma=False)
```

```python
import functools

import jax
import jax.numpy as jnp
import numpy as np
from jax import lax
from jax.experimental import pallas as pl
from jax.experimental.pallas import tpu as pltpu
from jax.sharding import PartitionSpec as P

ROT_DIM = 64
LN_EPS = 1e-5
SEQS = 8
BLOCK = 16
MESH = pl.DeviceIdType.MESH
F32 = jnp.float32
BF16 = jnp.bfloat16


def rotary_table(n_pos, head_dim):
    inv_freq = 1.0 / (10000.0 ** (jnp.arange(0, ROT_DIM, 2).astype(F32) / ROT_DIM))
    angles = jnp.arange(n_pos).astype(F32)[:, None] * inv_freq[None, :]
    cos, sin = jnp.cos(angles), jnp.sin(angles)
    rest = head_dim - ROT_DIM
    cos = jnp.concatenate([jnp.repeat(cos, 2, axis=1), jnp.ones((n_pos, rest), F32)], axis=1)
    sin = jnp.stack([-sin, sin], axis=-1).reshape(n_pos, ROT_DIM)
    sin = jnp.concatenate([sin, jnp.zeros((n_pos, rest), F32)], axis=1)
    terms = []
    for table in (cos, sin):
        for _ in range(3):
            term = lax.reduce_precision(table, 8, 7)
            terms.append(term.astype(BF16))
            table = table - term
    return jnp.concatenate(terms, axis=1)


def normalise(hid, gain, bias):
    row_mean = jnp.mean(hid, axis=-1, keepdims=True)
    centered = hid - row_mean
    row_var = jnp.mean(centered * centered, axis=-1, keepdims=True)
    return centered * lax.rsqrt(row_var + LN_EPS) * gain + bias


def kernel(dims, cl_s, clv, tab, gain, bias, bout, bin_, x_hbm, k_hbm, v_hbm, wq, wk, wv, win, wo, wout,
           hid_out, k_out, v_out,
           w1, w2, hbuf, own, xown, xbuf, kbuf, vbuf, qkv, cs, ctx, mid, part, arecv, pair, b1r, b2r,
           w_sem, x_sem, xo_sem, kv_sem, kvo_sem, out_sem,
           a_send, a_recv, b1_send, b1_recv, b2_send, b2_recv, g1_send, g1_recv, g2_send, g2_recv, d_send, d_recv):
    n_layers, n_chunks, steps, heads, head_dim, d_model, d_ff = dims
    rows = steps * SEQS
    half = rows // 2
    own_rows = rows // 8
    sub = own_rows // 2
    width = heads * head_dim
    slots2 = k_hbm.shape[2]
    total = n_layers * n_chunks
    me = lax.axis_index("tp")
    core = lax.rem(me, 2)
    chip = lax.div(me, 2)
    left, right = lax.rem(me + 6, 8), lax.rem(me + 2, 8)
    mate = me + 1 - 2 * core
    chip_l, chip_r, chip_o = lax.rem(chip + 3, 4), lax.rem(chip + 1, 4), lax.rem(chip + 2, 4)
    mult = pl.multiple_of

    def block_of(q):
        return mult(q * own_rows, own_rows)

    def rows_of(q):
        return mult(core * half + q * own_rows, own_rows)

    def remote(src, dst, send, recv, dev):
        return pltpu.make_async_remote_copy(src_ref=src, dst_ref=dst, send_sem=send, recv_sem=recv,
                                            device_id={"tp": dev}, device_id_type=MESH)

    barrier = pltpu.get_barrier_semaphore()
    for dev in (left, right, mate):
        pl.semaphore_signal(barrier, inc=1, device_id={"tp": dev}, device_id_type=MESH)

    def weight_copies(layer):
        return [pltpu.make_async_copy(wq.at[layer], w1.at[layer, :, pl.ds(0, width)], w_sem.at[layer, 0]),
                pltpu.make_async_copy(wk.at[layer], w1.at[layer, :, pl.ds(width, width)], w_sem.at[layer, 1]),
                pltpu.make_async_copy(wv.at[layer], w1.at[layer, :, pl.ds(2 * width, width)], w_sem.at[layer, 2]),
                pltpu.make_async_copy(win.at[layer], w1.at[layer, :, pl.ds(3 * width, d_ff)], w_sem.at[layer, 3]),
                pltpu.make_async_copy(wo.at[layer], w2.at[layer, pl.ds(0, width), :], w_sem.at[layer, 4]),
                pltpu.make_async_copy(wout.at[layer], w2.at[layer, pl.ds(width, d_ff), :], w_sem.at[layer, 5])]

    def x_copy(c):
        return pltpu.make_async_copy(x_hbm.at[:, pl.ds(mult(c * SEQS, SEQS), SEQS), :], xbuf.at[lax.rem(c, 2)],
                                     x_sem.at[lax.rem(c, 2)])

    def kv_in(i):
        layer, c, s = lax.div(i, n_chunks), lax.rem(i, n_chunks), lax.rem(i, 2)
        seqs = pl.ds(mult(c * SEQS, SEQS), SEQS)
        return [pltpu.make_async_copy(k_hbm.at[layer, seqs], kbuf.at[s], kv_sem.at[0, s]),
                pltpu.make_async_copy(v_hbm.at[layer, seqs], vbuf.at[s], kv_sem.at[1, s])]

    def kv_back(i):
        layer, c, s = lax.div(i, n_chunks), lax.rem(i, n_chunks), lax.rem(i, 2)
        seqs = pl.ds(mult(c * SEQS, SEQS), SEQS)
        return [pltpu.make_async_copy(kbuf.at[s], k_out.at[layer, seqs], kvo_sem.at[0, s]),
                pltpu.make_async_copy(vbuf.at[s], v_out.at[layer, seqs], kvo_sem.at[1, s])]

    def hid_copy(c):
        return pltpu.make_async_copy(hbuf.at[c], hid_out.at[c], out_sem.at[c])

    steps_own = own_rows // SEQS
    own_copy = pltpu.make_async_copy(x_hbm.at[pl.ds((core * 4 + chip) * steps_own, steps_own)], xown, xo_sem)
    x_copy(0).start()
    for copy in weight_copies(0)[:3]:
        copy.start()
    for copy in kv_in(0):
        copy.start()
    for copy in weight_copies(0)[3:]:
        copy.start()
    own_copy.start()
    for layer in range(1, n_layers):
        for copy in weight_copies(layer):
            copy.start()
    pl.semaphore_wait(barrier, 3)

    def piece_qkv(i):
        layer, c = lax.div(i, n_chunks), lax.rem(i, n_chunks)

        @pl.when(i >= 1)
        def _():
            for copy in kv_back(i - 1):
                copy.wait()

        @pl.when(i + 1 < total)
        def _():
            for copy in kv_in(i + 1):
                copy.start()

        @pl.when(i + 1 < n_chunks)
        def _():
            x_copy(i + 1).start()

        @pl.when(i < n_chunks)
        def _():
            x_copy(i).wait()
            s = lax.rem(c, 2)
            per = BLOCK // SEQS

            def block(j, carry):
                hid = xbuf[s, pl.ds(j * per, per)].astype(F32).reshape(BLOCK, d_model)
                normed = normalise(hid, gain[0].astype(F32), bias[0].astype(F32))
                hbuf[c, pl.ds(mult(j * BLOCK, BLOCK), BLOCK)] = normed.astype(BF16)
                return carry

            lax.fori_loop(0, rows // BLOCK, block, 0)

        for layer_w in range(n_layers):
            @pl.when(i == layer_w * n_chunks)
            def _(layer_w=layer_w):
                for copy in weight_copies(layer_w)[:3]:
                    copy.wait()

        pos = clv[pl.ds(mult(c * SEQS, SEQS), SEQS)][None] + lax.broadcasted_iota(jnp.int32, (steps, SEQS, 128), 0)
        pos = pos.reshape(rows, 128)
        pick = (pos == lax.broadcasted_iota(jnp.int32, (rows, 128), 1)).astype(F32).astype(BF16)
        tabs = jnp.dot(pick, tab[...], preferred_element_type=F32)
        e = head_dim
        cs[:, 0:e] = (tabs[:, 0:e] + tabs[:, e:2 * e]) + tabs[:, 2 * e:3 * e]
        cs[:, e:2 * e] = (tabs[:, 3 * e:4 * e] + tabs[:, 4 * e:5 * e]) + tabs[:, 5 * e:6 * e]
        even = lax.rem(lax.broadcasted_iota(jnp.int32, (rows, e), 1), 2) == 0
        qk = jnp.dot(hbuf[c], w1[layer, :, pl.ds(0, 2 * width)], preferred_element_type=F32)
        for h in range(2 * heads):
            vec = qk[:, h * e:(h + 1) * e]
            other = jnp.where(even, pltpu.roll(vec, e - 1, 1), pltpu.roll(vec, 1, 1))
            qkv[h] = vec * cs[:, 0:e] + other * cs[:, e:2 * e]
        val = jnp.dot(hbuf[c], w1[layer, :, pl.ds(2 * width, width)], preferred_element_type=F32)
        for h in range(heads):
            qkv[2 * heads + h] = val[:, h * e:(h + 1) * e]

    def piece_attend(i):
        layer, c, s = lax.div(i, n_chunks), lax.rem(i, n_chunks), lax.rem(i, 2)
        for copy in kv_in(i):
            copy.wait()
        e = head_dim
        ht = heads * steps
        scale = head_dim ** -0.5
        r_iota = lax.broadcasted_iota(jnp.int32, (slots2, ht), 0)
        j_iota = lax.broadcasted_iota(jnp.int32, (slots2, ht), 1)
        lag = r_iota - heads * lax.rem(j_iota, steps) - lax.div(j_iota, steps)
        slot_row = lax.div(lax.broadcasted_iota(jnp.int32, (slots2, e), 0), heads)
        rr = lax.broadcasted_iota(jnp.int32, (ht, slots2), 1)
        jj = lax.broadcasted_iota(jnp.int32, (ht, slots2), 0)
        seen = jnp.where(lax.rem(rr, heads) == lax.div(jj, steps), lax.div(rr, heads) - lax.rem(jj, steps), 1 << 20)
        for b in range(SEQS):
            n = cl_s[c * SEQS + b]

            def split(first):
                return jnp.concatenate([qkv[first + h, pl.ds(b, steps, stride=SEQS), :] for h in range(heads)],
                                       axis=0).astype(BF16)

            query, key, value = split(0), split(heads), split(2 * heads)
            place = (lag == heads * n).astype(F32).astype(BF16)
            placed = jnp.dot(place, jnp.concatenate([key, value], axis=1), preferred_element_type=F32).astype(BF16)
            fresh = (slot_row >= n) & (slot_row < n + steps)
            k_all = jnp.where(fresh, placed[:, 0:e], kbuf[s, b])
            v_all = jnp.where(fresh, placed[:, e:2 * e], vbuf[s, b])
            kbuf[s, b] = k_all
            vbuf[s, b] = v_all
            scores = lax.dot_general(query, k_all, (((1,), (1,)), ((), ())), preferred_element_type=F32) * scale
            scores = jnp.where(seen <= n, scores, -jnp.inf)
            exp_scores = jnp.exp(scores - jnp.max(scores, axis=-1, keepdims=True))
            probs = (exp_scores / jnp.sum(exp_scores, axis=-1, keepdims=True)).astype(BF16)
            context = jnp.dot(probs, v_all, preferred_element_type=F32)
            for h in range(heads):
                ctx[h, pl.ds(b, steps, stride=SEQS), :] = context[h * steps:(h + 1) * steps]
        for h in range(heads):
            mid[:, h * e:(h + 1) * e] = ctx[h].astype(BF16)
        for copy in kv_back(i):
            copy.start()

    def piece_ff(i):
        layer, c = lax.div(i, n_chunks), lax.rem(i, n_chunks)
        for layer_w in range(n_layers):
            @pl.when(i == layer_w * n_chunks)
            def _(layer_w=layer_w):
                weight_copies(layer_w)[3].wait()
        tile = 512

        def block(j, carry):
            cols = mult(j * tile, tile)
            pre = jnp.dot(hbuf[c], w1[layer, :, pl.ds(mult(3 * width + cols, 256), tile)], preferred_element_type=F32)
            pre = pre + bin_[layer, :, pl.ds(cols, tile)].astype(F32)
            inner = 0.7978845608028654 * (pre + 0.044715 * (pre * pre * pre))
            mid[:, pl.ds(mult(width + cols, 256), tile)] = (pre * (0.5 * (1.0 + jnp.tanh(inner)))).astype(BF16)
            return carry

        lax.fori_loop(0, d_ff // tile, block, 0)

    def piece_out(i):
        layer, s = lax.div(i, n_chunks), lax.rem(i, 2)
        for layer_w in range(n_layers):
            @pl.when(i == layer_w * n_chunks)
            def _(layer_w=layer_w):
                for copy in weight_copies(layer_w)[4:]:
                    copy.wait()
        tile = 512

        def block(j, carry):
            cols = pl.ds(mult(j * tile, tile), tile)
            part[s, :, cols] = jnp.dot(mid[...], w2[layer, :, cols], preferred_element_type=F32).astype(BF16)
            return carry

        lax.fori_loop(0, d_model // tile, block, 0)
        copy_a(i).start()

    def copy_a(u):
        s2, s4 = lax.rem(u, 2), lax.rem(u, 4)
        return remote(part.at[s2, pl.ds(mult((1 - core) * half, half), half)], arecv.at[s4], a_send.at[s2], a_recv.at[s4], mate)

    def copies_b1(u):
        c, s4 = lax.rem(u, n_chunks), lax.rem(u, 4)
        return [remote(pair.at[s4, pl.ds(block_of(chip_o), sub)], b1r.at[0, c], b1_send.at[0, c], b1_recv.at[0, c], left),
                remote(pair.at[s4, pl.ds(mult(block_of(chip_o) + sub, sub), sub)], b1r.at[1, c], b1_send.at[1, c],
                       b1_recv.at[1, c], right)]

    def copies_b2(u):
        c, s4 = lax.rem(u, n_chunks), lax.rem(u, 4)
        return [remote(pair.at[s4, pl.ds(block_of(chip_l), own_rows)], b2r.at[0, c], b2_send.at[0, c], b2_recv.at[0, c], left),
                remote(pair.at[s4, pl.ds(block_of(chip_r), own_rows)], b2r.at[1, c], b2_send.at[1, c], b2_recv.at[1, c], right)]

    def same_rows(c, start, size, send, recv, dev):
        ref = hbuf.at[c, pl.ds(start, size)]
        return remote(ref, ref, send, recv, dev)

    def copies_g1(u):
        c = lax.rem(u, n_chunks)
        mine = rows_of(chip)
        return [same_rows(c, mine, own_rows, g1_send.at[0, c], g1_recv.at[0, c], left),
                same_rows(c, mine, own_rows, g1_send.at[1, c], g1_recv.at[1, c], right),
                same_rows(c, mine, own_rows, d_send.at[0, c], d_recv.at[0, c], mate)]

    def copies_g2(u):
        c = lax.rem(u, n_chunks)
        from_r, from_l = rows_of(chip_r), rows_of(chip_l)
        return [same_rows(c, mult(from_r + sub, sub), sub, g2_send.at[0, c], g2_recv.at[0, c], left),
                same_rows(c, from_l, sub, g2_send.at[1, c], g2_recv.at[1, c], right),
                same_rows(c, from_r, own_rows, d_send.at[1, c], d_recv.at[1, c], mate),
                same_rows(c, from_l, own_rows, d_send.at[2, c], d_recv.at[2, c], mate)]

    def copy_g3(u):
        c = lax.rem(u, n_chunks)
        return same_rows(c, rows_of(chip_o), own_rows, d_send.at[3, c], d_recv.at[3, c], mate)

    def stage_b1(u):
        s2, s4 = lax.rem(u, 2), lax.rem(u, 4)
        copy_a(u).wait()

        def add(start):
            src = pl.ds(mult(core * half + start, BLOCK), BLOCK)
            dst = pl.ds(mult(start, BLOCK), BLOCK)
            pair[s4, dst] = (part[s2, src].astype(F32) + arecv[s4, dst].astype(F32)).astype(BF16)

        for t in range(own_rows // BLOCK):
            add(block_of(chip_o) + t * BLOCK)
        for copy in copies_b1(u):
            copy.start()
        for q in (chip_l, chip_r, chip):
            for t in range(own_rows // BLOCK):
                add(block_of(q) + t * BLOCK)

    def stage_b2(u):
        c, s4 = lax.rem(u, n_chunks), lax.rem(u, 4)
        first, second = copies_b1(u), copies_b2(u)
        first[0].wait_recv()
        dst = pl.ds(block_of(chip_l), sub)
        pair[s4, dst] = (pair[s4, dst].astype(F32) + b1r[0, c].astype(F32)).astype(BF16)
        second[0].start()
        first[1].wait_recv()
        dst = pl.ds(mult(block_of(chip_r) + sub, sub), sub)
        pair[s4, dst] = (pair[s4, dst].astype(F32) + b1r[1, c].astype(F32)).astype(BF16)
        second[1].start()

    def stage_b3(u):
        layer, c, s4 = lax.div(u, n_chunks), lax.rem(u, n_chunks), lax.rem(u, 4)
        for copy in copies_b2(u):
            copy.wait_recv()
        for t in range(own_rows // BLOCK):
            src = pl.ds(mult(block_of(chip) + t * BLOCK, BLOCK), BLOCK)
            loc = pl.ds(t * BLOCK, BLOCK)
            hid = own[c, loc].astype(F32) + bout[layer].astype(F32)
            hid = hid + (pair[s4, src].astype(F32) + (b2r[0, c, loc].astype(F32) + b2r[1, c, loc].astype(F32)))
            hid = hid.astype(BF16)
            dst = pl.ds(mult(rows_of(chip) + t * BLOCK, BLOCK), BLOCK)

            @pl.when(layer + 1 < n_layers)
            def _():
                own[c, loc] = hid
                nxt = layer + 1
                hbuf[c, dst] = normalise(hid.astype(F32), gain[nxt].astype(F32), bias[nxt].astype(F32)).astype(BF16)

            @pl.when(layer + 1 >= n_layers)
            def _():
                hbuf[c, dst] = hid

        for copy in copies_g1(u):
            copy.start()
        for copy in copies_b1(u) + copies_b2(u):
            copy.wait_send()

    def stage_g2(u):
        first, second = copies_g1(u), copies_g2(u)
        c = lax.rem(u, n_chunks)
        same_rows(c, rows_of(chip_r), own_rows, g1_send.at[0, c], g1_recv.at[0, c], left).wait_recv()
        second[0].start()
        second[2].start()
        same_rows(c, rows_of(chip_l), own_rows, g1_send.at[1, c], g1_recv.at[1, c], right).wait_recv()
        second[1].start()
        second[3].start()

    def stage_g3(u):
        c = lax.rem(u, n_chunks)
        theirs = rows_of(chip_o)
        same_rows(c, mult(theirs + sub, sub), sub, g2_send.at[0, c], g2_recv.at[0, c], left).wait_recv()
        same_rows(c, theirs, sub, g2_send.at[1, c], g2_recv.at[1, c], right).wait_recv()
        copy_g3(u).start()

    def stage_g4(u):
        c = lax.rem(u, n_chunks)
        for n, q in enumerate((chip, chip_r, chip_l, chip_o)):
            start = mult((1 - core) * half + q * own_rows, own_rows)
            same_rows(c, start, own_rows, d_send.at[n, c], d_recv.at[n, c], mate).wait_recv()
        for copy in copies_g1(u) + copies_g2(u) + [copy_g3(u)]:
            copy.wait_send()

        @pl.when(u >= total - n_chunks)
        def _():
            hid_copy(c).start()

    def guarded(stage, u):
        @pl.when((u >= 0) & (u < total))
        def _():
            stage(u)

    own_copy.wait()
    for c in range(n_chunks):
        own[c] = xown[:, c * SEQS:(c + 1) * SEQS].astype(F32).reshape(own_rows, d_model).astype(BF16)

    def tick(i, carry):
        guarded(stage_g2, i - 4)
        guarded(piece_qkv, i)
        guarded(stage_b3, i - 3)
        guarded(stage_g3, i - 5)
        guarded(piece_attend, i)
        guarded(stage_b2, i - 2)
        guarded(stage_g4, i - 6)
        guarded(piece_ff, i)
        guarded(stage_b1, i - 1)
        guarded(piece_out, i)
        return carry

    lax.fori_loop(0, total + 6, tick, 0)
    for copy in kv_back(total - 1):
        copy.wait()
    for c in range(n_chunks):
        hid_copy(c).wait()


def decode_shard(x_steps, cur_len, k_cache, v_cache, ln_gain, ln_bias, w_q, w_k, w_v, w_o, w_in, b_in, w_out, b_out):
    steps, batch, d_model = x_steps.shape
    n_layers, _, slots, heads, head_dim = k_cache.shape
    d_ff = w_in.shape[2]
    n_chunks = batch // SEQS
    rows = steps * SEQS
    width = heads * head_dim
    own_rows = rows // 8
    tab = rotary_table(128, head_dim)
    cl_rows = jnp.broadcast_to(cur_len[:, None], (batch, 128))
    k_rows = k_cache.reshape(n_layers, batch, slots * heads, head_dim)
    v_rows = v_cache.reshape(n_layers, batch, slots * heads, head_dim)
    vmem = pl.BlockSpec(memory_space=pltpu.VMEM)
    hbm = pl.BlockSpec(memory_space=pl.ANY)
    dims = (n_layers, n_chunks, steps, heads, head_dim, d_model, d_ff)
    dma = pltpu.SemaphoreType.DMA
    hid, k_new, v_new = pl.pallas_call(
        functools.partial(kernel, dims),
        out_shape=(jax.ShapeDtypeStruct((n_chunks, rows, d_model), BF16),
                   jax.ShapeDtypeStruct(k_rows.shape, BF16), jax.ShapeDtypeStruct(v_rows.shape, BF16)),
        in_specs=[pl.BlockSpec(memory_space=pltpu.SMEM)] + [vmem] * 6 + [hbm] * 9,
        out_specs=(hbm, hbm, hbm),
        scratch_shapes=[
            pltpu.VMEM((n_layers, d_model, 3 * width + d_ff), BF16),
            pltpu.VMEM((n_layers, width + d_ff, d_model), BF16),
            pltpu.VMEM((n_chunks, rows, d_model), BF16),
            pltpu.VMEM((n_chunks, own_rows, d_model), BF16),
            pltpu.VMEM((own_rows // SEQS, batch, d_model), BF16),
            pltpu.VMEM((2, steps, SEQS, d_model), BF16),
            pltpu.VMEM((2, SEQS, slots * heads, head_dim), BF16),
            pltpu.VMEM((2, SEQS, slots * heads, head_dim), BF16),
            pltpu.VMEM((3 * heads, rows, head_dim), F32),
            pltpu.VMEM((rows, 2 * head_dim), F32),
            pltpu.VMEM((heads, rows, head_dim), F32),
            pltpu.VMEM((rows, width + d_ff), BF16),
            pltpu.VMEM((2, rows, d_model), BF16),
            pltpu.VMEM((4, rows // 2, d_model), BF16),
            pltpu.VMEM((4, rows // 2, d_model), BF16),
            pltpu.VMEM((2, n_chunks, own_rows // 2, d_model), BF16),
            pltpu.VMEM((2, n_chunks, own_rows, d_model), BF16),
            dma((n_layers, 6)), dma((2,)), dma, dma((2, 2)), dma((2, 2)), dma((n_chunks,)),
            dma((2,)), dma((4,)), dma((2, n_chunks)), dma((2, n_chunks)), dma((2, n_chunks)), dma((2, n_chunks)),
            dma((2, n_chunks)), dma((2, n_chunks)), dma((2, n_chunks)), dma((2, n_chunks)),
            dma((4, n_chunks)), dma((4, n_chunks)),
        ],
        compiler_params=pltpu.CompilerParams(collective_id=0, has_side_effects=True, vmem_limit_bytes=67043328),
    )(cur_len, cl_rows, tab, ln_gain[:, None, :], ln_bias[:, None, :], b_out[:, None, :], b_in[:, None, :], x_steps, k_rows, v_rows,
      w_q, w_k, w_v, w_in, w_o, w_out)
    hidden = hid.reshape(n_chunks, steps, SEQS, d_model).transpose(1, 0, 2, 3).reshape(steps, batch, d_model)
    return hidden, k_new.reshape(k_cache.shape), v_new.reshape(v_cache.shape)


def solution(mesh):
    cache_spec = P(None, "dp", None, "tp", None)
    in_specs = (P(None, "dp", None), P("dp"), cache_spec, cache_spec, P(None, None), P(None, None),
                P(None, None, "tp"), P(None, None, "tp"), P(None, None, "tp"), P(None, "tp", None),
                P(None, None, "tp"), P(None, "tp"), P(None, "tp", None), P(None, None))
    out_specs = (P(None, "dp", None), cache_spec, cache_spec)
    return jax.shard_map(decode_shard, mesh=mesh, in_specs=in_specs, out_specs=out_specs, check_vma=False)
```

```python
import functools

import jax
import jax.numpy as jnp
import numpy as np
from jax import lax
from jax.experimental import pallas as pl
from jax.experimental.pallas import tpu as pltpu
from jax.sharding import PartitionSpec as P

ROT_DIM = 64
LN_EPS = 1e-5
SEQS = 8
GROUP = 8
BLOCK = 16
SCHEDULE = (("qkv", 0), ("b1", 1), ("g2", 3), ("g4", 4), ("mid", 0), ("b3", 2), ("out", 0), ("b2", 1), ("g3", 3))
MESH = pl.DeviceIdType.MESH
F32 = jnp.float32
BF16 = jnp.bfloat16


def rotary_table(n_pos, head_dim):
    inv_freq = (1.0 / np.power(10000.0, np.arange(0, ROT_DIM, 2) / ROT_DIM)).astype(np.float32)
    angles = (np.arange(n_pos, dtype=np.float32)[:, None] * inv_freq[None, :]).astype(np.float64)
    cos, sin = np.repeat(np.cos(angles), 2, axis=1), np.repeat(np.sin(angles), 2, axis=1)
    sin[:, 0::2] *= -1.0
    rest = head_dim - ROT_DIM
    cos = np.concatenate([cos, np.ones((n_pos, rest))], axis=1).astype(np.float32)
    sin = np.concatenate([sin, np.zeros((n_pos, rest))], axis=1).astype(np.float32)
    terms = []
    for table in (cos, sin):
        for _ in range(3):
            term = table.astype(BF16)
            terms.append(term)
            table = table - term.astype(np.float32)
    return np.concatenate(terms, axis=1)


def normalise(hid, gain, bias):
    row_mean = jnp.mean(hid, axis=-1, keepdims=True)
    centered = hid - row_mean
    row_var = jnp.mean(centered * centered, axis=-1, keepdims=True)
    return centered * lax.rsqrt(row_var + LN_EPS) * gain + bias


def kernel(dims, cl_s, tab, gain_in, bias_in, bout_in, bin_in, x_hbm, k_hbm, v_hbm, wq, wk, wv, win, wo, wout,
           hid_out, k_out, v_out,
           gain, bias, bout, bin_, w1, w2, hbuf, own, xown, xbuf, kbuf, vbuf, qkv, cs, ctx, mid, part, arecv, pair, b1r, b2r,
           w_sem, x_sem, xo_sem, kv_sem, kvo_sem, out_sem,
           a_send, a_recv, b1_send, b1_recv, b2_send, b2_recv, g1_send, g1_recv, g2_send, g2_recv, d_send, d_recv,
           bd_send, bd_recv, gn_send, gn_recv):
    n_layers, n_chunks, steps, heads, head_dim, d_model, d_ff = dims
    rows = steps * SEQS
    half = rows // 2
    own_rows = rows // 8
    sub = own_rows // 2
    width = heads * head_dim
    slots2 = k_hbm.shape[2]
    total = n_layers * n_chunks
    me = lax.axis_index("tp")
    core = lax.rem(me, 2)
    chip = lax.div(me, 2)
    left, right = lax.rem(me + 6, 8), lax.rem(me + 2, 8)
    mate = me + 1 - 2 * core
    chip_l, chip_r, chip_o = lax.rem(chip + 3, 4), lax.rem(chip + 1, 4), lax.rem(chip + 2, 4)
    mult = pl.multiple_of

    def block_of(q):
        return mult(q * own_rows, own_rows)

    def rows_of(q):
        return mult(core * half + q * own_rows, own_rows)

    def remote(src, dst, send, recv, dev):
        return pltpu.make_async_remote_copy(src_ref=src, dst_ref=dst, send_sem=send, recv_sem=recv,
                                            device_id={"tp": dev}, device_id_type=MESH)

    barrier = pltpu.get_barrier_semaphore()
    for dev in (left, right, mate):
        pl.semaphore_signal(barrier, inc=1, device_id={"tp": dev}, device_id_type=MESH)

    def weight_copies(layer):
        return [pltpu.make_async_copy(wq.at[layer], w1.at[layer, :, pl.ds(0, width)], w_sem.at[layer, 0]),
                pltpu.make_async_copy(wk.at[layer], w1.at[layer, :, pl.ds(width, width)], w_sem.at[layer, 1]),
                pltpu.make_async_copy(wv.at[layer], w1.at[layer, :, pl.ds(2 * width, width)], w_sem.at[layer, 2]),
                pltpu.make_async_copy(win.at[layer], w1.at[layer, :, pl.ds(3 * width, d_ff)], w_sem.at[layer, 3]),
                pltpu.make_async_copy(wo.at[layer], w2.at[layer, pl.ds(0, width), :], w_sem.at[layer, 4]),
                pltpu.make_async_copy(wout.at[layer], w2.at[layer, pl.ds(width, d_ff), :], w_sem.at[layer, 5])]

    def x_copy(c):
        return pltpu.make_async_copy(x_hbm.at[:, pl.ds(mult(c * SEQS, SEQS), SEQS), :], xbuf.at[lax.rem(c, 2)],
                                     x_sem.at[lax.rem(c, 2)])

    def kv_in(i):
        layer, c, s = lax.div(i, n_chunks), lax.rem(i, n_chunks), lax.rem(i, 2)
        seqs = pl.ds(mult(c * SEQS, SEQS), SEQS)
        return [pltpu.make_async_copy(k_hbm.at[layer, seqs], kbuf.at[s], kv_sem.at[0, s]),
                pltpu.make_async_copy(v_hbm.at[layer, seqs], vbuf.at[s], kv_sem.at[1, s])]

    def kv_back(i):
        layer, c, s = lax.div(i, n_chunks), lax.rem(i, n_chunks), lax.rem(i, 2)
        seqs = pl.ds(mult(c * SEQS, SEQS), SEQS)
        return [pltpu.make_async_copy(kbuf.at[s], k_out.at[layer, seqs], kvo_sem.at[0, s]),
                pltpu.make_async_copy(vbuf.at[s], v_out.at[layer, seqs], kvo_sem.at[1, s])]

    def hid_copy(c):
        return pltpu.make_async_copy(hbuf.at[c], hid_out.at[c], out_sem.at[c])

    steps_own = own_rows // SEQS
    own_copy = pltpu.make_async_copy(x_hbm.at[pl.ds((core * 4 + chip) * steps_own, steps_own)], xown, xo_sem)
    x_copy(0).start()
    for copy in weight_copies(0)[:3]:
        copy.start()
    for copy in kv_in(0):
        copy.start()
    for copy in weight_copies(0)[3:]:
        copy.start()
    own_copy.start()

    for layer in range(n_layers):
        for dst, src in ((gain, gain_in), (bias, bias_in), (bout, bout_in), (bin_, bin_in)):
            dst[layer] = src[layer:layer + 1].astype(F32)

    def piece_qkv(i):
        layer, c = lax.div(i, n_chunks), lax.rem(i, n_chunks)

        @pl.when(i >= 1)
        def _():
            for copy in kv_back(i - 1):
                copy.wait()

        @pl.when(i + 1 < total)
        def _():
            for copy in kv_in(i + 1):
                copy.start()

        @pl.when(i + 1 < n_chunks)
        def _():
            x_copy(i + 1).start()

        @pl.when(i < n_chunks)
        def _():
            x_copy(i).wait()
            s = lax.rem(c, 2)
            per = BLOCK // SEQS

            def block(j, carry):
                hid = xbuf[s, pl.ds(j * per, per)].astype(F32).reshape(BLOCK, d_model)
                normed = normalise(hid, gain[0], bias[0])
                hbuf[c, pl.ds(mult(j * BLOCK, BLOCK), BLOCK)] = normed.astype(BF16)
                return carry

            lax.fori_loop(0, rows // BLOCK, block, 0, unroll=8)

        for layer_w in range(n_layers):
            @pl.when(i == layer_w * n_chunks)
            def _(layer_w=layer_w):
                for copy in weight_copies(layer_w)[:3]:
                    copy.wait()

        row = lax.broadcasted_iota(jnp.int32, (rows, 128), 0)
        pos = lax.div(row, SEQS)
        for b in range(SEQS):
            pos = pos + jnp.where(lax.rem(row, SEQS) == b, cl_s[c * SEQS + b], 0)
        pick = (pos == lax.broadcasted_iota(jnp.int32, (rows, 128), 1)).astype(F32).astype(BF16)
        tabs = jnp.dot(pick, tab[...], preferred_element_type=F32)
        e = head_dim
        cs[:, 0:e] = (tabs[:, 0:e] + tabs[:, e:2 * e]) + tabs[:, 2 * e:3 * e]
        cs[:, e:2 * e] = (tabs[:, 3 * e:4 * e] + tabs[:, 4 * e:5 * e]) + tabs[:, 5 * e:6 * e]
        even = lax.rem(lax.broadcasted_iota(jnp.int32, (rows, e), 1), 2) == 0
        qk = jnp.dot(hbuf[c], w1[layer, :, pl.ds(0, 2 * width)], preferred_element_type=F32)
        for h in range(2 * heads):
            vec = qk[:, h * e:(h + 1) * e]
            other = jnp.where(even, pltpu.roll(vec, e - 1, 1), pltpu.roll(vec, 1, 1))
            qkv[h] = vec * cs[:, 0:e] + other * cs[:, e:2 * e]
        val = jnp.dot(hbuf[c], w1[layer, :, pl.ds(2 * width, width)], preferred_element_type=F32)
        for h in range(heads):
            qkv[2 * heads + h] = val[:, h * e:(h + 1) * e]

    def piece_mid(i):
        for layer_w in range(n_layers):
            @pl.when(i == layer_w * n_chunks)
            def _(layer_w=layer_w):
                for copy in weight_copies(layer_w)[3:]:
                    copy.wait()

        piece_ff(i)
        piece_attend(i)

    def piece_attend(i):
        layer, c, s = lax.div(i, n_chunks), lax.rem(i, n_chunks), lax.rem(i, 2)
        for copy in kv_in(i):
            copy.wait()
        e = head_dim
        ht = heads * steps
        scale = head_dim ** -0.5
        r_iota = lax.broadcasted_iota(jnp.int32, (slots2, ht), 0)
        j_iota = lax.broadcasted_iota(jnp.int32, (slots2, ht), 1)
        lag = r_iota - heads * lax.rem(j_iota, steps) - lax.div(j_iota, steps)
        slot_row = lax.div(lax.broadcasted_iota(jnp.int32, (slots2, e), 0), heads)
        rr = lax.broadcasted_iota(jnp.int32, (ht, slots2), 1)
        jj = lax.broadcasted_iota(jnp.int32, (ht, slots2), 0)
        seen = jnp.where(lax.rem(rr, heads) == lax.div(jj, steps), lax.div(rr, heads) - lax.rem(jj, steps), 1 << 20)

        def split(b, first):
            return jnp.concatenate([qkv[first + h, pl.ds(b, steps, stride=SEQS), :] for h in range(heads)], axis=0).astype(BF16)

        for g in range(0, SEQS, GROUP):
            group = range(g, g + GROUP)
            lens = [cl_s[c * SEQS + b] for b in group]
            placed = [jnp.dot((lag == heads * n).astype(F32).astype(BF16),
                              jnp.concatenate([split(b, heads), split(b, 2 * heads)], axis=1),
                              preferred_element_type=F32).astype(BF16) for b, n in zip(group, lens)]
            queries = [split(b, 0) for b in group]
            fresh = [(slot_row >= n) & (slot_row < n + steps) for n in lens]
            k_all = [jnp.where(f, p[:, 0:e], kbuf[s, b]) for b, f, p in zip(group, fresh, placed)]
            v_all = [jnp.where(f, p[:, e:2 * e], vbuf[s, b]) for b, f, p in zip(group, fresh, placed)]
            scores = [lax.dot_general(q, k, (((1,), (1,)), ((), ())), preferred_element_type=F32) * scale
                      for q, k in zip(queries, k_all)]
            for b, k, v in zip(group, k_all, v_all):
                kbuf[s, b] = k
                vbuf[s, b] = v
            scores = [jnp.where(seen <= n, sc, -jnp.inf) for sc, n in zip(scores, lens)]
            exps = [jnp.exp(sc - jnp.max(sc, axis=-1, keepdims=True)) for sc in scores]
            probs = [(ex / jnp.sum(ex, axis=-1, keepdims=True)).astype(BF16) for ex in exps]
            contexts = [jnp.dot(p, v, preferred_element_type=F32) for p, v in zip(probs, v_all)]
            for b, context in zip(group, contexts):
                for h in range(heads):
                    ctx[h, pl.ds(b, steps, stride=SEQS), :] = context[h * steps:(h + 1) * steps]
        for h in range(heads):
            mid[:, h * e:(h + 1) * e] = ctx[h].astype(BF16)
        for copy in kv_back(i):
            copy.start()

    def piece_ff(i):
        layer, c = lax.div(i, n_chunks), lax.rem(i, n_chunks)
        tile = 512

        def block(j, carry):
            cols = mult(j * tile, tile)
            pre = jnp.dot(hbuf[c], w1[layer, :, pl.ds(mult(3 * width + cols, 256), tile)], preferred_element_type=F32)
            pre = pre + bin_[layer, :, pl.ds(cols, tile)]
            inner = 0.7978845608028654 * (pre + 0.044715 * (pre * pre * pre))
            mid[:, pl.ds(mult(width + cols, 256), tile)] = (pre * (0.5 * (1.0 + jnp.tanh(inner)))).astype(BF16)
            return carry

        lax.fori_loop(0, d_ff // tile, block, 0, unroll=True)

    def piece_out(i):
        layer, s = lax.div(i, n_chunks), lax.rem(i, 2)
        tile = 512

        def block(j, carry):
            cols = pl.ds(mult(j * tile, tile), tile)
            part[s, :, cols] = jnp.dot(mid[...], w2[layer, :, cols], preferred_element_type=F32).astype(BF16)
            return carry

        lax.fori_loop(0, d_model // tile, block, 0, unroll=True)
        copy_a(i).start()

    def copy_a(u):
        s2, s4 = lax.rem(u, 2), lax.rem(u, 4)
        return remote(part.at[s2, pl.ds(mult((1 - core) * half, half), half)], arecv.at[s4], a_send.at[s2], a_recv.at[s4], mate)

    def copies_b1(u):
        c, s4 = lax.rem(u, n_chunks), lax.rem(u, 4)
        return [remote(pair.at[s4, pl.ds(block_of(chip_o), sub)], b1r.at[0, c], b1_send.at[0, c], b1_recv.at[0, c], left),
                remote(pair.at[s4, pl.ds(mult(block_of(chip_o) + sub, sub), sub)], b1r.at[1, c], b1_send.at[1, c],
                       b1_recv.at[1, c], right)]

    def copies_bd(u):
        c, s4 = lax.rem(u, n_chunks), lax.rem(u, 4)
        return [remote(pair.at[s4, pl.ds(mult(block_of(chip_l) + sub, sub), sub)], b2r.at[0, c, pl.ds(sub, sub)],
                       bd_send.at[0, c], bd_recv.at[0, c], left),
                remote(pair.at[s4, pl.ds(block_of(chip_r), sub)], b2r.at[1, c, pl.ds(0, sub)],
                       bd_send.at[1, c], bd_recv.at[1, c], right)]

    def copies_b2(u):
        c, s4 = lax.rem(u, n_chunks), lax.rem(u, 4)
        return [remote(pair.at[s4, pl.ds(block_of(chip_l), sub)], b2r.at[0, c, pl.ds(0, sub)],
                       b2_send.at[0, c], b2_recv.at[0, c], left),
                remote(pair.at[s4, pl.ds(mult(block_of(chip_r) + sub, sub), sub)], b2r.at[1, c, pl.ds(sub, sub)],
                       b2_send.at[1, c], b2_recv.at[1, c], right)]

    def same_rows(c, start, size, send, recv, dev):
        ref = hbuf.at[c, pl.ds(start, size)]
        return remote(ref, ref, send, recv, dev)

    def copies_g1(u):
        c = lax.rem(u, n_chunks)
        mine = rows_of(chip)
        other = mult(mine + sub, sub)
        return [same_rows(c, other, sub, g1_send.at[0, c], g1_recv.at[0, c], left),
                same_rows(c, mine, sub, g1_send.at[1, c], g1_recv.at[1, c], right),
                same_rows(c, mine, sub, gn_send.at[0, c], gn_recv.at[0, c], left),
                same_rows(c, other, sub, gn_send.at[1, c], gn_recv.at[1, c], right),
                same_rows(c, mine, own_rows, d_send.at[0, c], d_recv.at[0, c], mate)]

    def copies_g2(u):
        c = lax.rem(u, n_chunks)
        from_r, from_l = rows_of(chip_r), rows_of(chip_l)
        return [same_rows(c, mult(from_r + sub, sub), sub, g2_send.at[0, c], g2_recv.at[0, c], left),
                same_rows(c, from_l, sub, g2_send.at[1, c], g2_recv.at[1, c], right),
                same_rows(c, from_r, own_rows, d_send.at[1, c], d_recv.at[1, c], mate),
                same_rows(c, from_l, own_rows, d_send.at[2, c], d_recv.at[2, c], mate)]

    def copy_g3(u):
        c = lax.rem(u, n_chunks)
        return same_rows(c, rows_of(chip_o), own_rows, d_send.at[3, c], d_recv.at[3, c], mate)

    def stage_b1(u):
        s2, s4 = lax.rem(u, 2), lax.rem(u, 4)
        copy_a(u).wait()

        def add(start):
            src = pl.ds(mult(core * half + start, BLOCK), BLOCK)
            dst = pl.ds(mult(start, BLOCK), BLOCK)
            pair[s4, dst] = (part[s2, src].astype(F32) + arecv[s4, dst].astype(F32)).astype(BF16)

        for t in range(own_rows // BLOCK):
            add(block_of(chip_o) + t * BLOCK)
        for copy in copies_b1(u):
            copy.start()
        add(block_of(chip_l) + sub)
        add(block_of(chip_r))
        for copy in copies_bd(u):
            copy.start()
        add(block_of(chip_l))
        add(block_of(chip_r) + sub)
        for t in range(own_rows // BLOCK):
            add(block_of(chip) + t * BLOCK)

    def stage_b2(u):
        c, s4 = lax.rem(u, n_chunks), lax.rem(u, 4)
        first, second = copies_b1(u), copies_b2(u)
        first[0].wait_recv()
        dst = pl.ds(block_of(chip_l), sub)
        pair[s4, dst] = (pair[s4, dst].astype(F32) + b1r[0, c].astype(F32)).astype(BF16)
        second[0].start()
        first[1].wait_recv()
        dst = pl.ds(mult(block_of(chip_r) + sub, sub), sub)
        pair[s4, dst] = (pair[s4, dst].astype(F32) + b1r[1, c].astype(F32)).astype(BF16)
        second[1].start()

    def stage_b3(u):
        layer, c, s4 = lax.div(u, n_chunks), lax.rem(u, n_chunks), lax.rem(u, 4)
        for copy in copies_bd(u) + copies_b2(u):
            copy.wait_recv()
        for t in range(own_rows // BLOCK):
            src = pl.ds(mult(block_of(chip) + t * BLOCK, BLOCK), BLOCK)
            loc = pl.ds(t * BLOCK, BLOCK)
            hid = own[c, loc].astype(F32) + bout[layer]
            hid = hid + (pair[s4, src].astype(F32) + (b2r[0, c, loc].astype(F32) + b2r[1, c, loc].astype(F32)))
            hid = hid.astype(BF16)
            dst = pl.ds(mult(rows_of(chip) + t * BLOCK, BLOCK), BLOCK)

            @pl.when(layer + 1 < n_layers)
            def _():
                own[c, loc] = hid
                nxt = layer + 1
                hbuf[c, dst] = normalise(hid.astype(F32), gain[nxt], bias[nxt]).astype(BF16)

            @pl.when(layer + 1 >= n_layers)
            def _():
                hbuf[c, dst] = hid

        for copy in copies_g1(u):
            copy.start()

    def stage_g2(u):
        second = copies_g2(u)
        c = lax.rem(u, n_chunks)
        from_r, from_l = rows_of(chip_r), rows_of(chip_l)
        same_rows(c, mult(from_r + sub, sub), sub, g1_send.at[0, c], g1_recv.at[0, c], left).wait_recv()
        second[0].start()
        same_rows(c, from_l, sub, g1_send.at[1, c], g1_recv.at[1, c], right).wait_recv()
        second[1].start()
        same_rows(c, from_r, sub, gn_send.at[0, c], gn_recv.at[0, c], left).wait_recv()
        second[2].start()
        same_rows(c, mult(from_l + sub, sub), sub, gn_send.at[1, c], gn_recv.at[1, c], right).wait_recv()
        second[3].start()

    def stage_g3(u):
        c = lax.rem(u, n_chunks)
        theirs = rows_of(chip_o)
        same_rows(c, mult(theirs + sub, sub), sub, g2_send.at[0, c], g2_recv.at[0, c], left).wait_recv()
        same_rows(c, theirs, sub, g2_send.at[1, c], g2_recv.at[1, c], right).wait_recv()
        copy_g3(u).start()
        for copy in copies_b1(u) + copies_bd(u) + copies_b2(u):
            copy.wait_send()

    def stage_g4(u):
        c = lax.rem(u, n_chunks)
        for n, q in enumerate((chip, chip_r, chip_l, chip_o)):
            start = mult((1 - core) * half + q * own_rows, own_rows)
            same_rows(c, start, own_rows, d_send.at[n, c], d_recv.at[n, c], mate).wait_recv()
        for copy in copies_g1(u) + copies_g2(u) + [copy_g3(u)]:
            copy.wait_send()

        @pl.when(u >= total - n_chunks)
        def _():
            hid_copy(c).start()

    def guarded(stage, u):
        @pl.when((u >= 0) & (u < total))
        def _():
            stage(u)

    parts = {"qkv": piece_qkv, "mid": piece_mid, "out": piece_out, "b1": stage_b1, "b2": stage_b2, "b3": stage_b3,
             "g2": stage_g2, "g3": stage_g3, "g4": stage_g4}

    def greet():
        pl.semaphore_wait(barrier, 3)

    def fetch():
        for layer in range(1, n_layers):
            for copy in weight_copies(layer):
                copy.start()
        own_copy.wait()
        for c in range(n_chunks):
            own[c] = xown[:, c * SEQS:(c + 1) * SEQS].astype(F32).reshape(own_rows, d_model).astype(BF16)

    def tick(i, carry):
        for name, lag in SCHEDULE:
            guarded(parts[name], i - lag)
            if name == "qkv":
                pl.when(i == 0)(greet)
                pl.when(i == 1)(fetch)
        return carry

    lax.fori_loop(0, total + max(lag for _, lag in SCHEDULE), tick, 0)
    for copy in kv_back(total - 1):
        copy.wait()
    for c in range(n_chunks):
        hid_copy(c).wait()


def deliver(hid, k_new, v_new, hid_out, k_out, v_out, hid_buf, kv_buf, in_sem, out_sem):
    n_chunks, _, seqs, _ = hid.shape
    n_layers, batch = k_new.shape[:2]
    size = kv_buf.shape[1]
    moves = [(src.at[layer, pl.ds(b, size)], None, dst.at[layer, pl.ds(b, size)])
             for src, dst in ((k_new, k_out), (v_new, v_out)) for layer in range(n_layers) for b in range(0, batch, size)]
    moves = [(src, kv_buf.at[n], dst) for n, (src, _, dst) in enumerate(moves)]
    moves += [(hid.at[c], hid_buf.at[c], hid_out.at[:, pl.ds(c * seqs, seqs), :]) for c in range(n_chunks)]
    takes = [pltpu.make_async_copy(src, buf, in_sem.at[n]) for n, (src, buf, _) in enumerate(moves)]
    gives = [pltpu.make_async_copy(buf, dst, out_sem.at[n]) for n, (_, buf, dst) in enumerate(moves)]
    for copy in takes:
        copy.start()
    for take, give in zip(takes, gives):
        take.wait()
        give.start()
    for copy in gives:
        copy.wait()


def decode_shard(x_steps, cur_len, k_cache, v_cache, ln_gain, ln_bias, w_q, w_k, w_v, w_o, w_in, b_in, w_out, b_out):
    steps, batch, d_model = x_steps.shape
    n_layers, _, slots, heads, head_dim = k_cache.shape
    d_ff = w_in.shape[2]
    n_chunks = batch // SEQS
    rows = steps * SEQS
    width = heads * head_dim
    own_rows = rows // 8
    tab = rotary_table(128, head_dim)
    k_rows = k_cache.reshape(n_layers, batch, slots * heads, head_dim)
    v_rows = v_cache.reshape(n_layers, batch, slots * heads, head_dim)
    vmem = pl.BlockSpec(memory_space=pltpu.VMEM)
    hbm = pl.BlockSpec(memory_space=pl.ANY)
    dims = (n_layers, n_chunks, steps, heads, head_dim, d_model, d_ff)
    dma = pltpu.SemaphoreType.DMA
    hid, k_new, v_new = pl.pallas_call(
        functools.partial(kernel, dims),
        out_shape=(jax.ShapeDtypeStruct((n_chunks, rows, d_model), BF16),
                   jax.ShapeDtypeStruct(k_rows.shape, BF16), jax.ShapeDtypeStruct(v_rows.shape, BF16)),
        in_specs=[pl.BlockSpec(memory_space=pltpu.SMEM)] + [vmem] * 5 + [hbm] * 9,
        out_specs=(hbm, hbm, hbm),
        scratch_shapes=[
            pltpu.VMEM((n_layers, 1, d_model), F32),
            pltpu.VMEM((n_layers, 1, d_model), F32),
            pltpu.VMEM((n_layers, 1, d_model), F32),
            pltpu.VMEM((n_layers, 1, d_ff), F32),
            pltpu.VMEM((n_layers, d_model, 3 * width + d_ff), BF16),
            pltpu.VMEM((n_layers, width + d_ff, d_model), BF16),
            pltpu.VMEM((n_chunks, rows, d_model), BF16),
            pltpu.VMEM((n_chunks, own_rows, d_model), BF16),
            pltpu.VMEM((own_rows // SEQS, batch, d_model), BF16),
            pltpu.VMEM((2, steps, SEQS, d_model), BF16),
            pltpu.VMEM((2, SEQS, slots * heads, head_dim), BF16),
            pltpu.VMEM((2, SEQS, slots * heads, head_dim), BF16),
            pltpu.VMEM((3 * heads, rows, head_dim), F32),
            pltpu.VMEM((rows, 2 * head_dim), F32),
            pltpu.VMEM((heads, rows, head_dim), F32),
            pltpu.VMEM((rows, width + d_ff), BF16),
            pltpu.VMEM((2, rows, d_model), BF16),
            pltpu.VMEM((4, rows // 2, d_model), BF16),
            pltpu.VMEM((4, rows // 2, d_model), BF16),
            pltpu.VMEM((2, n_chunks, own_rows // 2, d_model), BF16),
            pltpu.VMEM((2, n_chunks, own_rows, d_model), BF16),
            dma((n_layers, 6)), dma((2,)), dma, dma((2, 2)), dma((2, 2)), dma((n_chunks,)),
            dma((2,)), dma((4,)), dma((2, n_chunks)), dma((2, n_chunks)), dma((2, n_chunks)), dma((2, n_chunks)),
            dma((2, n_chunks)), dma((2, n_chunks)), dma((2, n_chunks)), dma((2, n_chunks)),
            dma((4, n_chunks)), dma((4, n_chunks)),
            dma((2, n_chunks)), dma((2, n_chunks)), dma((2, n_chunks)), dma((2, n_chunks)),
        ],
        compiler_params=pltpu.CompilerParams(collective_id=0, has_side_effects=True, vmem_limit_bytes=67043328),
    )(cur_len, tab, ln_gain, ln_bias, b_out, b_in, x_steps, k_rows, v_rows,
      w_q, w_k, w_v, w_in, w_o, w_out)
    size = 16
    pieces = 2 * n_layers * batch // size
    hidden, k_new, v_new = pl.pallas_call(
        deliver,
        out_shape=(jax.ShapeDtypeStruct(x_steps.shape, BF16),
                   jax.ShapeDtypeStruct(k_rows.shape, BF16), jax.ShapeDtypeStruct(v_rows.shape, BF16)),
        in_specs=[hbm] * 3,
        out_specs=(hbm, hbm, hbm),
        scratch_shapes=[pltpu.VMEM((n_chunks, steps, SEQS, d_model), BF16),
                        pltpu.VMEM((pieces, size, slots * heads, head_dim), BF16),
                        dma((pieces + n_chunks,)), dma((pieces + n_chunks,))],
        compiler_params=pltpu.CompilerParams(vmem_limit_bytes=67043328),
    )(hid.reshape(n_chunks, steps, SEQS, d_model), k_new, v_new)
    return hidden, k_new.reshape(k_cache.shape), v_new.reshape(v_cache.shape)


def solution(mesh):
    cache_spec = P(None, "dp", None, "tp", None)
    in_specs = (P(None, "dp", None), P("dp"), cache_spec, cache_spec, P(None, None), P(None, None),
                P(None, None, "tp"), P(None, None, "tp"), P(None, None, "tp"), P(None, "tp", None),
                P(None, None, "tp"), P(None, "tp"), P(None, "tp", None), P(None, None))
    out_specs = (P(None, "dp", None), cache_spec, cache_spec)
    return jax.shard_map(decode_shard, mesh=mesh, in_specs=in_specs, out_specs=out_specs, check_vma=False)
```

```python
import functools

import jax
import jax.numpy as jnp
import numpy as np
from jax import lax
from jax.experimental import pallas as pl
from jax.experimental.pallas import tpu as pltpu
from jax.sharding import PartitionSpec as P

ROT_DIM = 64
LN_EPS = 1e-5
SEQS = 8
GROUP = 8
BLOCK = 16
SCHEDULE = (("qkv", 0), ("b1", 1), ("g2", 3), ("g4", 4), ("mid", 0), ("b3", 2), ("out", 0), ("b2", 1), ("g3", 3))
MESH = pl.DeviceIdType.MESH
F32 = jnp.float32
BF16 = jnp.bfloat16


def rotary_table(n_pos, head_dim):
    inv_freq = (1.0 / np.power(10000.0, np.arange(0, ROT_DIM, 2) / ROT_DIM)).astype(np.float32)
    angles = (np.arange(n_pos, dtype=np.float32)[:, None] * inv_freq[None, :]).astype(np.float64)
    cos, sin = np.repeat(np.cos(angles), 2, axis=1), np.repeat(np.sin(angles), 2, axis=1)
    sin[:, 0::2] *= -1.0
    rest = head_dim - ROT_DIM
    cos = np.concatenate([cos, np.ones((n_pos, rest))], axis=1).astype(np.float32)
    sin = np.concatenate([sin, np.zeros((n_pos, rest))], axis=1).astype(np.float32)
    terms = []
    for table in (cos, sin):
        for _ in range(3):
            term = table.astype(BF16)
            terms.append(term)
            table = table - term.astype(np.float32)
    return np.concatenate(terms, axis=1)


def normalise(hid, gain, bias):
    row_mean = jnp.mean(hid, axis=-1, keepdims=True)
    centered = hid - row_mean
    row_var = jnp.mean(centered * centered, axis=-1, keepdims=True)
    return centered * lax.rsqrt(row_var + LN_EPS) * gain + bias


def kernel(dims, cl_s, tab, gain_in, bias_in, bout_in, bin_in, x_hbm, k_hbm, v_hbm, wq, wk, wv, win, wo, wout,
           hbuf, k_out, v_out,
           gain, bias, bout, bin_, w1, w2, own, xown, xbuf, kbuf, vbuf, qkv, cs, ctx, mid, part, arecv, pair, b1r, b2r,
           w_sem, x_sem, xo_sem, kv_sem,
           a_send, a_recv, b1_send, b1_recv, b2_send, b2_recv, g1_send, g1_recv, g2_send, g2_recv, d_send, d_recv,
           bd_send, bd_recv, gn_send, gn_recv):
    n_layers, n_chunks, steps, heads, head_dim, d_model, d_ff = dims
    rows = steps * SEQS
    half = rows // 2
    own_rows = rows // 8
    sub = own_rows // 2
    width = heads * head_dim
    slots2 = k_hbm.shape[2]
    total = n_layers * n_chunks
    me = lax.axis_index("tp")
    core = lax.rem(me, 2)
    chip = lax.div(me, 2)
    left, right = lax.rem(me + 6, 8), lax.rem(me + 2, 8)
    mate = me + 1 - 2 * core
    chip_l, chip_r, chip_o = lax.rem(chip + 3, 4), lax.rem(chip + 1, 4), lax.rem(chip + 2, 4)
    mult = pl.multiple_of

    def block_of(q):
        return mult(q * own_rows, own_rows)

    def rows_of(q):
        return mult(core * half + q * own_rows, own_rows)

    def remote(src, dst, send, recv, dev):
        return pltpu.make_async_remote_copy(src_ref=src, dst_ref=dst, send_sem=send, recv_sem=recv,
                                            device_id={"tp": dev}, device_id_type=MESH)

    barrier = pltpu.get_barrier_semaphore()
    for dev in (left, right, mate):
        pl.semaphore_signal(barrier, inc=1, device_id={"tp": dev}, device_id_type=MESH)

    def weight_copies(layer):
        return [pltpu.make_async_copy(wq.at[layer], w1.at[:, pl.ds(0, width)], w_sem.at[0]),
                pltpu.make_async_copy(wk.at[layer], w1.at[:, pl.ds(width, width)], w_sem.at[1]),
                pltpu.make_async_copy(wv.at[layer], w1.at[:, pl.ds(2 * width, width)], w_sem.at[2]),
                pltpu.make_async_copy(win.at[layer], w1.at[:, pl.ds(3 * width, d_ff)], w_sem.at[3]),
                pltpu.make_async_copy(wo.at[layer], w2.at[pl.ds(0, width), :], w_sem.at[4]),
                pltpu.make_async_copy(wout.at[layer], w2.at[pl.ds(width, d_ff), :], w_sem.at[5])]

    def x_copy(c):
        return pltpu.make_async_copy(x_hbm.at[:, pl.ds(mult(c * SEQS, SEQS), SEQS), :], xbuf.at[lax.rem(c, 2)],
                                     x_sem.at[lax.rem(c, 2)])

    def kv_in(i):
        layer, c, s = lax.div(i, n_chunks), lax.rem(i, n_chunks), lax.rem(i, 2)
        seqs = pl.ds(mult(c * SEQS, SEQS), SEQS)
        return [pltpu.make_async_copy(k_hbm.at[layer, seqs], kbuf.at[s], kv_sem.at[0, s]),
                pltpu.make_async_copy(v_hbm.at[layer, seqs], vbuf.at[s], kv_sem.at[1, s])]

    steps_own = own_rows // SEQS
    own_copy = pltpu.make_async_copy(x_hbm.at[pl.ds((core * 4 + chip) * steps_own, steps_own)], xown, xo_sem)
    x_copy(0).start()
    for copy in weight_copies(0)[:3]:
        copy.start()
    for copy in kv_in(0):
        copy.start()
    for copy in weight_copies(0)[3:]:
        copy.start()
    own_copy.start()

    for layer in range(n_layers):
        for dst, src in ((gain, gain_in), (bias, bias_in), (bout, bout_in), (bin_, bin_in)):
            dst[layer] = src[layer:layer + 1].astype(F32)

    def take_weights(i, lo, hi):
        @pl.when(lax.rem(i, n_chunks) == 0)
        def _():
            for copy in weight_copies(lax.div(i, n_chunks))[lo:hi]:
                copy.wait()

    def next_weights(i, lo, hi):
        @pl.when((lax.rem(i, n_chunks) == n_chunks - 1) & (i + 1 < total))
        def _():
            for copy in weight_copies(lax.div(i, n_chunks) + 1)[lo:hi]:
                copy.start()

    def piece_qkv(i):
        layer, c = lax.div(i, n_chunks), lax.rem(i, n_chunks)

        @pl.when(i + 1 < total)
        def _():
            for copy in kv_in(i + 1):
                copy.start()

        @pl.when(i + 1 < n_chunks)
        def _():
            x_copy(i + 1).start()

        @pl.when(i < n_chunks)
        def _():
            x_copy(i).wait()
            s = lax.rem(c, 2)
            per = BLOCK // SEQS

            def block(j, carry):
                hid = xbuf[s, pl.ds(j * per, per)].astype(F32).reshape(BLOCK, d_model)
                normed = normalise(hid, gain[0], bias[0])
                hbuf[c, pl.ds(mult(j * BLOCK, BLOCK), BLOCK)] = normed.astype(BF16)
                return carry

            lax.fori_loop(0, rows // BLOCK, block, 0, unroll=8)

        take_weights(i, 0, 3)

        row = lax.broadcasted_iota(jnp.int32, (rows, 128), 0)
        pos = lax.div(row, SEQS)
        for b in range(SEQS):
            pos = pos + jnp.where(lax.rem(row, SEQS) == b, cl_s[c * SEQS + b], 0)
        pick = (pos == lax.broadcasted_iota(jnp.int32, (rows, 128), 1)).astype(F32).astype(BF16)
        tabs = jnp.dot(pick, tab[...], preferred_element_type=F32)
        e = head_dim
        cs[:, 0:e] = (tabs[:, 0:e] + tabs[:, e:2 * e]) + tabs[:, 2 * e:3 * e]
        cs[:, e:2 * e] = (tabs[:, 3 * e:4 * e] + tabs[:, 4 * e:5 * e]) + tabs[:, 5 * e:6 * e]
        even = lax.rem(lax.broadcasted_iota(jnp.int32, (rows, e), 1), 2) == 0
        qk = jnp.dot(hbuf[c], w1[:, pl.ds(0, 2 * width)], preferred_element_type=F32)
        for h in range(2 * heads):
            vec = qk[:, h * e:(h + 1) * e]
            other = jnp.where(even, pltpu.roll(vec, e - 1, 1), pltpu.roll(vec, 1, 1))
            qkv[h] = vec * cs[:, 0:e] + other * cs[:, e:2 * e]
        val = jnp.dot(hbuf[c], w1[:, pl.ds(2 * width, width)], preferred_element_type=F32)
        for h in range(heads):
            qkv[2 * heads + h] = val[:, h * e:(h + 1) * e]
        next_weights(i, 0, 3)

    def piece_mid(i):
        take_weights(i, 3, 6)

        piece_ff(i)
        piece_attend(i)
        next_weights(i, 3, 4)

    def piece_attend(i):
        layer, c, s = lax.div(i, n_chunks), lax.rem(i, n_chunks), lax.rem(i, 2)
        for copy in kv_in(i):
            copy.wait()
        e = head_dim
        ht = heads * steps
        scale = head_dim ** -0.5
        r_iota = lax.broadcasted_iota(jnp.int32, (slots2, ht), 0)
        j_iota = lax.broadcasted_iota(jnp.int32, (slots2, ht), 1)
        lag = r_iota - heads * lax.rem(j_iota, steps) - lax.div(j_iota, steps)
        slot_row = lax.div(lax.broadcasted_iota(jnp.int32, (slots2, e), 0), heads)
        rr = lax.broadcasted_iota(jnp.int32, (ht, slots2), 1)
        jj = lax.broadcasted_iota(jnp.int32, (ht, slots2), 0)
        seen = jnp.where(lax.rem(rr, heads) == lax.div(jj, steps), lax.div(rr, heads) - lax.rem(jj, steps), 1 << 20)

        def split(b, first):
            return jnp.concatenate([qkv[first + h, pl.ds(b, steps, stride=SEQS), :] for h in range(heads)], axis=0).astype(BF16)

        for g in range(0, SEQS, GROUP):
            group = range(g, g + GROUP)
            lens = [cl_s[c * SEQS + b] for b in group]
            placed = [jnp.dot((lag == heads * n).astype(F32).astype(BF16),
                              jnp.concatenate([split(b, heads), split(b, 2 * heads)], axis=1),
                              preferred_element_type=F32).astype(BF16) for b, n in zip(group, lens)]
            queries = [split(b, 0) for b in group]
            fresh = [(slot_row >= n) & (slot_row < n + steps) for n in lens]
            k_all = [jnp.where(f, p[:, 0:e], kbuf[s, b]) for b, f, p in zip(group, fresh, placed)]
            v_all = [jnp.where(f, p[:, e:2 * e], vbuf[s, b]) for b, f, p in zip(group, fresh, placed)]
            scores = [lax.dot_general(q, k, (((1,), (1,)), ((), ())), preferred_element_type=F32) * scale
                      for q, k in zip(queries, k_all)]
            for b, k, v in zip(group, k_all, v_all):
                k_out[layer, c * SEQS + b] = k
                v_out[layer, c * SEQS + b] = v
            scores = [jnp.where(seen <= n, sc, -jnp.inf) for sc, n in zip(scores, lens)]
            exps = [jnp.exp(sc - jnp.max(sc, axis=-1, keepdims=True)) for sc in scores]
            probs = [(ex / jnp.sum(ex, axis=-1, keepdims=True)).astype(BF16) for ex in exps]
            contexts = [jnp.dot(p, v, preferred_element_type=F32) for p, v in zip(probs, v_all)]
            for b, context in zip(group, contexts):
                for h in range(heads):
                    ctx[h, pl.ds(b, steps, stride=SEQS), :] = context[h * steps:(h + 1) * steps]
        for h in range(heads):
            mid[:, h * e:(h + 1) * e] = ctx[h].astype(BF16)

    def piece_ff(i):
        layer, c = lax.div(i, n_chunks), lax.rem(i, n_chunks)
        tile = 512

        def block(j, carry):
            cols = mult(j * tile, tile)
            pre = jnp.dot(hbuf[c], w1[:, pl.ds(mult(3 * width + cols, 256), tile)], preferred_element_type=F32)
            pre = pre + bin_[layer, :, pl.ds(cols, tile)]
            inner = 0.7978845608028654 * (pre + 0.044715 * (pre * pre * pre))
            mid[:, pl.ds(mult(width + cols, 256), tile)] = (pre * (0.5 * (1.0 + jnp.tanh(inner)))).astype(BF16)
            return carry

        lax.fori_loop(0, d_ff // tile, block, 0, unroll=True)

    def piece_out(i):
        layer, s = lax.div(i, n_chunks), lax.rem(i, 2)
        tile = 512

        def block(j, carry):
            cols = pl.ds(mult(j * tile, tile), tile)
            part[s, :, cols] = jnp.dot(mid[...], w2[:, cols], preferred_element_type=F32).astype(BF16)
            return carry

        lax.fori_loop(0, d_model // tile, block, 0, unroll=True)
        copy_a(i).start()
        next_weights(i, 4, 6)

    def copy_a(u):
        s2, s4 = lax.rem(u, 2), lax.rem(u, 4)
        return remote(part.at[s2, pl.ds(mult((1 - core) * half, half), half)], arecv.at[s4], a_send.at[s2], a_recv.at[s4], mate)

    def copies_b1(u):
        c, s4 = lax.rem(u, n_chunks), lax.rem(u, 4)
        return [remote(pair.at[s4, pl.ds(block_of(chip_o), sub)], b1r.at[0, c], b1_send.at[0, c], b1_recv.at[0, c], left),
                remote(pair.at[s4, pl.ds(mult(block_of(chip_o) + sub, sub), sub)], b1r.at[1, c], b1_send.at[1, c],
                       b1_recv.at[1, c], right)]

    def copies_bd(u):
        c, s4 = lax.rem(u, n_chunks), lax.rem(u, 4)
        return [remote(pair.at[s4, pl.ds(mult(block_of(chip_l) + sub, sub), sub)], b2r.at[0, c, pl.ds(sub, sub)],
                       bd_send.at[0, c], bd_recv.at[0, c], left),
                remote(pair.at[s4, pl.ds(block_of(chip_r), sub)], b2r.at[1, c, pl.ds(0, sub)],
                       bd_send.at[1, c], bd_recv.at[1, c], right)]

    def copies_b2(u):
        c, s4 = lax.rem(u, n_chunks), lax.rem(u, 4)
        return [remote(pair.at[s4, pl.ds(block_of(chip_l), sub)], b2r.at[0, c, pl.ds(0, sub)],
                       b2_send.at[0, c], b2_recv.at[0, c], left),
                remote(pair.at[s4, pl.ds(mult(block_of(chip_r) + sub, sub), sub)], b2r.at[1, c, pl.ds(sub, sub)],
                       b2_send.at[1, c], b2_recv.at[1, c], right)]

    def same_rows(c, start, size, send, recv, dev):
        ref = hbuf.at[c, pl.ds(start, size)]
        return remote(ref, ref, send, recv, dev)

    def copies_g1(u):
        c = lax.rem(u, n_chunks)
        mine = rows_of(chip)
        other = mult(mine + sub, sub)
        return [same_rows(c, other, sub, g1_send.at[0, c], g1_recv.at[0, c], left),
                same_rows(c, mine, sub, g1_send.at[1, c], g1_recv.at[1, c], right),
                same_rows(c, mine, sub, gn_send.at[0, c], gn_recv.at[0, c], left),
                same_rows(c, other, sub, gn_send.at[1, c], gn_recv.at[1, c], right),
                same_rows(c, mine, own_rows, d_send.at[0, c], d_recv.at[0, c], mate)]

    def copies_g2(u):
        c = lax.rem(u, n_chunks)
        from_r, from_l = rows_of(chip_r), rows_of(chip_l)
        return [same_rows(c, mult(from_r + sub, sub), sub, g2_send.at[0, c], g2_recv.at[0, c], left),
                same_rows(c, from_l, sub, g2_send.at[1, c], g2_recv.at[1, c], right),
                same_rows(c, from_r, own_rows, d_send.at[1, c], d_recv.at[1, c], mate),
                same_rows(c, from_l, own_rows, d_send.at[2, c], d_recv.at[2, c], mate)]

    def copy_g3(u):
        c = lax.rem(u, n_chunks)
        return same_rows(c, rows_of(chip_o), own_rows, d_send.at[3, c], d_recv.at[3, c], mate)

    def stage_b1(u):
        s2, s4 = lax.rem(u, 2), lax.rem(u, 4)
        copy_a(u).wait()

        def add(start):
            src = pl.ds(mult(core * half + start, BLOCK), BLOCK)
            dst = pl.ds(mult(start, BLOCK), BLOCK)
            pair[s4, dst] = (part[s2, src].astype(F32) + arecv[s4, dst].astype(F32)).astype(BF16)

        for t in range(own_rows // BLOCK):
            add(block_of(chip_o) + t * BLOCK)
        for copy in copies_b1(u):
            copy.start()
        add(block_of(chip_l) + sub)
        add(block_of(chip_r))
        for copy in copies_bd(u):
            copy.start()
        add(block_of(chip_l))
        add(block_of(chip_r) + sub)
        for t in range(own_rows // BLOCK):
            add(block_of(chip) + t * BLOCK)

    def stage_b2(u):
        c, s4 = lax.rem(u, n_chunks), lax.rem(u, 4)
        first, second = copies_b1(u), copies_b2(u)
        first[0].wait_recv()
        dst = pl.ds(block_of(chip_l), sub)
        pair[s4, dst] = (pair[s4, dst].astype(F32) + b1r[0, c].astype(F32)).astype(BF16)
        second[0].start()
        first[1].wait_recv()
        dst = pl.ds(mult(block_of(chip_r) + sub, sub), sub)
        pair[s4, dst] = (pair[s4, dst].astype(F32) + b1r[1, c].astype(F32)).astype(BF16)
        second[1].start()

    def stage_b3(u):
        layer, c, s4 = lax.div(u, n_chunks), lax.rem(u, n_chunks), lax.rem(u, 4)
        for copy in copies_bd(u) + copies_b2(u):
            copy.wait_recv()
        for t in range(own_rows // BLOCK):
            src = pl.ds(mult(block_of(chip) + t * BLOCK, BLOCK), BLOCK)
            loc = pl.ds(t * BLOCK, BLOCK)
            hid = own[c, loc].astype(F32) + bout[layer]
            hid = hid + (pair[s4, src].astype(F32) + (b2r[0, c, loc].astype(F32) + b2r[1, c, loc].astype(F32)))
            hid = hid.astype(BF16)
            dst = pl.ds(mult(rows_of(chip) + t * BLOCK, BLOCK), BLOCK)

            @pl.when(layer + 1 < n_layers)
            def _():
                own[c, loc] = hid
                nxt = layer + 1
                hbuf[c, dst] = normalise(hid.astype(F32), gain[nxt], bias[nxt]).astype(BF16)

            @pl.when(layer + 1 >= n_layers)
            def _():
                hbuf[c, dst] = hid

        for copy in copies_g1(u):
            copy.start()

    def stage_g2(u):
        second = copies_g2(u)
        c = lax.rem(u, n_chunks)
        from_r, from_l = rows_of(chip_r), rows_of(chip_l)
        same_rows(c, mult(from_r + sub, sub), sub, g1_send.at[0, c], g1_recv.at[0, c], left).wait_recv()
        second[0].start()
        same_rows(c, from_l, sub, g1_send.at[1, c], g1_recv.at[1, c], right).wait_recv()
        second[1].start()
        same_rows(c, from_r, sub, gn_send.at[0, c], gn_recv.at[0, c], left).wait_recv()
        second[2].start()
        same_rows(c, mult(from_l + sub, sub), sub, gn_send.at[1, c], gn_recv.at[1, c], right).wait_recv()
        second[3].start()

    def stage_g3(u):
        c = lax.rem(u, n_chunks)
        theirs = rows_of(chip_o)
        same_rows(c, mult(theirs + sub, sub), sub, g2_send.at[0, c], g2_recv.at[0, c], left).wait_recv()
        same_rows(c, theirs, sub, g2_send.at[1, c], g2_recv.at[1, c], right).wait_recv()
        copy_g3(u).start()
        for copy in copies_b1(u) + copies_bd(u) + copies_b2(u):
            copy.wait_send()

    def stage_g4(u):
        c = lax.rem(u, n_chunks)
        for n, q in enumerate((chip, chip_r, chip_l, chip_o)):
            start = mult((1 - core) * half + q * own_rows, own_rows)
            same_rows(c, start, own_rows, d_send.at[n, c], d_recv.at[n, c], mate).wait_recv()
        for copy in copies_g1(u) + copies_g2(u) + [copy_g3(u)]:
            copy.wait_send()

    def guarded(stage, u):
        @pl.when((u >= 0) & (u < total))
        def _():
            stage(u)

    parts = {"qkv": piece_qkv, "mid": piece_mid, "out": piece_out, "b1": stage_b1, "b2": stage_b2, "b3": stage_b3,
             "g2": stage_g2, "g3": stage_g3, "g4": stage_g4}

    def greet():
        pl.semaphore_wait(barrier, 3)

    def fetch():
        own_copy.wait()
        for c in range(n_chunks):
            own[c] = xown[:, c * SEQS:(c + 1) * SEQS].astype(F32).reshape(own_rows, d_model).astype(BF16)

    def tick(i, carry):
        for name, lag in SCHEDULE:
            guarded(parts[name], i - lag)
            if name == "qkv":
                pl.when(i == 0)(greet)
                pl.when(i == 1)(fetch)
        return carry

    lax.fori_loop(0, total + max(lag for _, lag in SCHEDULE), tick, 0)


def deliver(hid, k_new, v_new, hid_out, k_out, v_out, out_sem):
    n_chunks, rows, d_model = hid.shape
    steps = hid_out.shape[0]
    seqs = rows // steps
    moves = [(hid.at[c].reshape(steps, seqs, d_model), hid_out.at[:, pl.ds(c * seqs, seqs), :]) for c in range(n_chunks)]
    for src, dst in ((k_new, k_out), (v_new, v_out)):
        n_layers, batch = src.shape[:2]
        size = batch // 4
        moves += [(src.at[layer, pl.ds(b, size)], dst.at[layer, pl.ds(b, size)])
                  for layer in range(n_layers) for b in range(0, batch, size)]
    copies = [pltpu.make_async_copy(src, dst, out_sem.at[n]) for n, (src, dst) in enumerate(moves)]
    for copy in copies:
        copy.start()
    for copy in copies:
        copy.wait()


def decode_shard(x_steps, cur_len, k_cache, v_cache, ln_gain, ln_bias, w_q, w_k, w_v, w_o, w_in, b_in, w_out, b_out):
    steps, batch, d_model = x_steps.shape
    n_layers, _, slots, heads, head_dim = k_cache.shape
    d_ff = w_in.shape[2]
    n_chunks = batch // SEQS
    rows = steps * SEQS
    width = heads * head_dim
    own_rows = rows // 8
    tab = rotary_table(128, head_dim)
    k_rows = k_cache.reshape(n_layers, batch, slots * heads, head_dim)
    v_rows = v_cache.reshape(n_layers, batch, slots * heads, head_dim)
    vmem = pl.BlockSpec(memory_space=pltpu.VMEM)
    hbm = pl.BlockSpec(memory_space=pl.ANY)
    dims = (n_layers, n_chunks, steps, heads, head_dim, d_model, d_ff)
    dma = pltpu.SemaphoreType.DMA
    hid, k_new, v_new = pl.pallas_call(
        functools.partial(kernel, dims),
        out_shape=(pltpu.VMEM((n_chunks, rows, d_model), BF16), pltpu.VMEM(k_rows.shape, BF16), pltpu.VMEM(v_rows.shape, BF16)),
        in_specs=[pl.BlockSpec(memory_space=pltpu.SMEM)] + [vmem] * 5 + [hbm] * 9,
        out_specs=(vmem, vmem, vmem),
        scratch_shapes=[
            pltpu.VMEM((n_layers, 1, d_model), F32),
            pltpu.VMEM((n_layers, 1, d_model), F32),
            pltpu.VMEM((n_layers, 1, d_model), F32),
            pltpu.VMEM((n_layers, 1, d_ff), F32),
            pltpu.VMEM((d_model, 3 * width + d_ff), BF16),
            pltpu.VMEM((width + d_ff, d_model), BF16),
            pltpu.VMEM((n_chunks, own_rows, d_model), BF16),
            pltpu.VMEM((own_rows // SEQS, batch, d_model), BF16),
            pltpu.VMEM((2, steps, SEQS, d_model), BF16),
            pltpu.VMEM((2, SEQS, slots * heads, head_dim), BF16),
            pltpu.VMEM((2, SEQS, slots * heads, head_dim), BF16),
            pltpu.VMEM((3 * heads, rows, head_dim), F32),
            pltpu.VMEM((rows, 2 * head_dim), F32),
            pltpu.VMEM((heads, rows, head_dim), F32),
            pltpu.VMEM((rows, width + d_ff), BF16),
            pltpu.VMEM((2, rows, d_model), BF16),
            pltpu.VMEM((4, rows // 2, d_model), BF16),
            pltpu.VMEM((4, rows // 2, d_model), BF16),
            pltpu.VMEM((2, n_chunks, own_rows // 2, d_model), BF16),
            pltpu.VMEM((2, n_chunks, own_rows, d_model), BF16),
            dma((6,)), dma((2,)), dma, dma((2, 2)),
            dma((2,)), dma((4,)), dma((2, n_chunks)), dma((2, n_chunks)), dma((2, n_chunks)), dma((2, n_chunks)),
            dma((2, n_chunks)), dma((2, n_chunks)), dma((2, n_chunks)), dma((2, n_chunks)),
            dma((4, n_chunks)), dma((4, n_chunks)),
            dma((2, n_chunks)), dma((2, n_chunks)), dma((2, n_chunks)), dma((2, n_chunks)),
        ],
        compiler_params=pltpu.CompilerParams(collective_id=0, has_side_effects=True, vmem_limit_bytes=38 * 2**20),
    )(cur_len, tab, ln_gain, ln_bias, b_out, b_in, x_steps, k_rows, v_rows,
      w_q, w_k, w_v, w_in, w_o, w_out)
    hidden, k_new, v_new = pl.pallas_call(
        deliver,
        out_shape=(jax.ShapeDtypeStruct(x_steps.shape, BF16),
                   jax.ShapeDtypeStruct(k_rows.shape, BF16), jax.ShapeDtypeStruct(v_rows.shape, BF16)),
        in_specs=[vmem] * 3,
        out_specs=(hbm, hbm, hbm),
        scratch_shapes=[dma((n_chunks + 8 * n_layers,))],
        compiler_params=pltpu.CompilerParams(vmem_limit_bytes=2**20),
    )(*[pltpu.with_memory_space_constraint(a, pltpu.VMEM) for a in (hid, k_new, v_new)])
    return hidden, k_new.reshape(k_cache.shape), v_new.reshape(v_cache.shape)


def solution(mesh):
    cache_spec = P(None, "dp", None, "tp", None)
    in_specs = (P(None, "dp", None), P("dp"), cache_spec, cache_spec, P(None, None), P(None, None),
                P(None, None, "tp"), P(None, None, "tp"), P(None, None, "tp"), P(None, "tp", None),
                P(None, None, "tp"), P(None, "tp"), P(None, "tp", None), P(None, None))
    out_specs = (P(None, "dp", None), cache_spec, cache_spec)
    return jax.shard_map(decode_shard, mesh=mesh, in_specs=in_specs, out_specs=out_specs, check_vma=False)
```

```python
import functools

import jax
import jax.numpy as jnp
import numpy as np
from jax import lax
from jax.experimental import pallas as pl
from jax.experimental.pallas import tpu as pltpu
from jax.sharding import PartitionSpec as P

ROT_DIM = 64
LN_EPS = 1e-5
SEQS = 8
GROUP = 8
BLOCK = 16
SCHEDULE = (("qkv", 0), ("b1", 1), ("g3", 4), ("mid", 0), ("att", 0), ("g2", 3), ("b3", 2), ("out", 0), ("b2", 1), ("g4", 4))
MESH = pl.DeviceIdType.MESH
F32 = jnp.float32
BF16 = jnp.bfloat16


def rotary_table(n_pos, head_dim):
    inv_freq = (1.0 / np.power(10000.0, np.arange(0, ROT_DIM, 2) / ROT_DIM)).astype(np.float32)
    angles = (np.arange(n_pos, dtype=np.float32)[:, None] * inv_freq[None, :]).astype(np.float64)
    cos, sin = np.repeat(np.cos(angles), 2, axis=1), np.repeat(np.sin(angles), 2, axis=1)
    sin[:, 0::2] *= -1.0
    rest = head_dim - ROT_DIM
    cos = np.concatenate([cos, np.ones((n_pos, rest))], axis=1).astype(np.float32)
    sin = np.concatenate([sin, np.zeros((n_pos, rest))], axis=1).astype(np.float32)
    terms = []
    for table in (cos, sin):
        for _ in range(3):
            term = table.astype(BF16)
            terms.append(term)
            table = table - term.astype(np.float32)
    return np.concatenate(terms, axis=1)


def normalise(hid, gain, bias):
    row_mean = jnp.mean(hid, axis=-1, keepdims=True)
    centered = hid - row_mean
    row_var = jnp.mean(centered * centered, axis=-1, keepdims=True)
    return centered * lax.rsqrt(row_var + LN_EPS) * gain + bias


def kernel(dims, cl_s, tab, gain_in, bias_in, bout_in, bin_in, x_hbm, k_hbm, v_hbm, wq, wk, wv, win, wo, wout,
           hbuf, k_out, v_out,
           gain, bias, bout, bin_, w1, w2, own, xown, xbuf, kbuf, vbuf, qkv, cs, ctx, mid, part, arecv, pair, b1r, b2r,
           w_sem, x_sem, xo_sem, kv_sem,
           a_send, a_recv, b1_send, b1_recv, b2_send, b2_recv, g1_send, g1_recv, g2_send, g2_recv, d_send, d_recv,
           bd_send, bd_recv, gn_send, gn_recv):
    n_layers, n_chunks, steps, heads, head_dim, d_model, d_ff = dims
    rows = steps * SEQS
    half = rows // 2
    own_rows = rows // 8
    sub = own_rows // 2
    width = heads * head_dim
    slots2 = k_hbm.shape[2]
    total = n_layers * n_chunks
    me = lax.axis_index("tp")
    core = lax.rem(me, 2)
    chip = lax.div(me, 2)
    left, right = lax.rem(me + 6, 8), lax.rem(me + 2, 8)
    mate = me + 1 - 2 * core
    chip_l, chip_r, chip_o = lax.rem(chip + 3, 4), lax.rem(chip + 1, 4), lax.rem(chip + 2, 4)
    mult = pl.multiple_of

    def block_of(q):
        return mult(q * own_rows, own_rows)

    def rows_of(q):
        return mult(core * half + q * own_rows, own_rows)

    def remote(src, dst, send, recv, dev):
        return pltpu.make_async_remote_copy(src_ref=src, dst_ref=dst, send_sem=send, recv_sem=recv,
                                            device_id={"tp": dev}, device_id_type=MESH)

    barrier = pltpu.get_barrier_semaphore()
    for dev in (left, right, mate):
        pl.semaphore_signal(barrier, inc=1, device_id={"tp": dev}, device_id_type=MESH)

    def weight_copies(layer):
        return [pltpu.make_async_copy(wq.at[layer], w1.at[:, pl.ds(0, width)], w_sem.at[0]),
                pltpu.make_async_copy(wk.at[layer], w1.at[:, pl.ds(width, width)], w_sem.at[1]),
                pltpu.make_async_copy(wv.at[layer], w1.at[:, pl.ds(2 * width, width)], w_sem.at[2]),
                pltpu.make_async_copy(win.at[layer], w1.at[:, pl.ds(3 * width, d_ff)], w_sem.at[3]),
                pltpu.make_async_copy(wo.at[layer], w2.at[pl.ds(0, width), :], w_sem.at[4]),
                pltpu.make_async_copy(wout.at[layer], w2.at[pl.ds(width, d_ff), :], w_sem.at[5])]

    def x_copy(c):
        return pltpu.make_async_copy(x_hbm.at[:, pl.ds(mult(c * SEQS, SEQS), SEQS), :], xbuf.at[lax.rem(c, 2)],
                                     x_sem.at[lax.rem(c, 2)])

    def kv_in(i):
        layer, c, s = lax.div(i, n_chunks), lax.rem(i, n_chunks), lax.rem(i, 2)
        seqs = pl.ds(mult(c * SEQS, SEQS), SEQS)
        return [pltpu.make_async_copy(k_hbm.at[layer, seqs], kbuf.at[s], kv_sem.at[0, s]),
                pltpu.make_async_copy(v_hbm.at[layer, seqs], vbuf.at[s], kv_sem.at[1, s])]

    steps_own = own_rows // SEQS
    own_copy = pltpu.make_async_copy(x_hbm.at[pl.ds((core * 4 + chip) * steps_own, steps_own)], xown, xo_sem)
    x_copy(0).start()
    for copy in weight_copies(0)[:3]:
        copy.start()
    for copy in kv_in(0):
        copy.start()
    for copy in weight_copies(0)[3:]:
        copy.start()
    own_copy.start()

    for layer in range(n_layers):
        for dst, src in ((gain, gain_in), (bias, bias_in), (bout, bout_in), (bin_, bin_in)):
            dst[layer] = src[layer:layer + 1].astype(F32)

    def take_weights(i, lo, hi):
        @pl.when(lax.rem(i, n_chunks) == 0)
        def _():
            for copy in weight_copies(lax.div(i, n_chunks))[lo:hi]:
                copy.wait()

    def next_weights(i, lo, hi):
        @pl.when((lax.rem(i, n_chunks) == n_chunks - 1) & (i + 1 < total))
        def _():
            for copy in weight_copies(lax.div(i, n_chunks) + 1)[lo:hi]:
                copy.start()

    def piece_qkv(i):
        layer, c = lax.div(i, n_chunks), lax.rem(i, n_chunks)

        @pl.when(i + 1 < total)
        def _():
            for copy in kv_in(i + 1):
                copy.start()

        @pl.when(i + 1 < n_chunks)
        def _():
            x_copy(i + 1).start()

        @pl.when(i < n_chunks)
        def _():
            x_copy(i).wait()
            s = lax.rem(c, 2)
            per = BLOCK // SEQS

            def block(j, carry):
                hid = xbuf[s, pl.ds(j * per, per)].astype(F32).reshape(BLOCK, d_model)
                normed = normalise(hid, gain[0], bias[0])
                hbuf[c, pl.ds(mult(j * BLOCK, BLOCK), BLOCK)] = normed.astype(BF16)
                return carry

            lax.fori_loop(0, rows // BLOCK, block, 0, unroll=8)

        take_weights(i, 0, 3)

        row = lax.broadcasted_iota(jnp.int32, (rows, 128), 0)
        pos = lax.div(row, SEQS)
        for b in range(SEQS):
            pos = pos + jnp.where(lax.rem(row, SEQS) == b, cl_s[c * SEQS + b], 0)
        pick = (pos == lax.broadcasted_iota(jnp.int32, (rows, 128), 1)).astype(F32).astype(BF16)
        tabs = jnp.dot(pick, tab[...], preferred_element_type=F32)
        e = head_dim
        cs[:, 0:e] = (tabs[:, 0:e] + tabs[:, e:2 * e]) + tabs[:, 2 * e:3 * e]
        cs[:, e:2 * e] = (tabs[:, 3 * e:4 * e] + tabs[:, 4 * e:5 * e]) + tabs[:, 5 * e:6 * e]
        even = lax.rem(lax.broadcasted_iota(jnp.int32, (rows, e), 1), 2) == 0
        qk = jnp.dot(hbuf[c], w1[:, pl.ds(0, 3 * width)], preferred_element_type=F32)
        for h in range(2 * heads):
            vec = qk[:, h * e:(h + 1) * e]
            other = jnp.where(even, pltpu.roll(vec, e - 1, 1), pltpu.roll(vec, 1, 1))
            qkv[h] = vec * cs[:, 0:e] + other * cs[:, e:2 * e]
        val = qk[:, 2 * width:3 * width]
        for h in range(heads):
            qkv[2 * heads + h] = val[:, h * e:(h + 1) * e]
        next_weights(i, 0, 3)

    def piece_mid(i):
        take_weights(i, 3, 6)

        piece_ff(i)
        next_weights(i, 3, 4)

    def piece_attend(i):
        layer, c, s = lax.div(i, n_chunks), lax.rem(i, n_chunks), lax.rem(i, 2)
        for copy in kv_in(i):
            copy.wait()
        e = head_dim
        ht = heads * steps
        scale = head_dim ** -0.5
        r_iota = lax.broadcasted_iota(jnp.int32, (slots2, ht), 0)
        j_iota = lax.broadcasted_iota(jnp.int32, (slots2, ht), 1)
        lag = r_iota - heads * lax.rem(j_iota, steps) - lax.div(j_iota, steps)
        slot_row = lax.div(lax.broadcasted_iota(jnp.int32, (slots2, e), 0), heads)
        rr = lax.broadcasted_iota(jnp.int32, (ht, slots2), 1)
        jj = lax.broadcasted_iota(jnp.int32, (ht, slots2), 0)
        seen = jnp.where(lax.rem(rr, heads) == lax.div(jj, steps), lax.div(rr, heads) - lax.rem(jj, steps), 1 << 20)

        def split(b, first):
            return jnp.concatenate([qkv[first + h, pl.ds(b, steps, stride=SEQS), :] for h in range(heads)], axis=0).astype(BF16)

        for g in range(0, SEQS, GROUP):
            group = range(g, g + GROUP)
            lens = [cl_s[c * SEQS + b] for b in group]
            placed = [jnp.dot((lag == heads * n).astype(F32).astype(BF16),
                              jnp.concatenate([split(b, heads), split(b, 2 * heads)], axis=1),
                              preferred_element_type=F32).astype(BF16) for b, n in zip(group, lens)]
            queries = [split(b, 0) for b in group]
            fresh = [(slot_row >= n) & (slot_row < n + steps) for n in lens]
            k_all = [jnp.where(f, p[:, 0:e], kbuf[s, b]) for b, f, p in zip(group, fresh, placed)]
            v_all = [jnp.where(f, p[:, e:2 * e], vbuf[s, b]) for b, f, p in zip(group, fresh, placed)]
            scores = [lax.dot_general(q, k, (((1,), (1,)), ((), ())), preferred_element_type=F32) * scale
                      for q, k in zip(queries, k_all)]
            for b, k, v in zip(group, k_all, v_all):
                k_out[layer, c * SEQS + b] = k
                v_out[layer, c * SEQS + b] = v
            scores = [jnp.where(seen <= n, sc, -jnp.inf) for sc, n in zip(scores, lens)]
            exps = [jnp.exp(sc - jnp.max(sc, axis=-1, keepdims=True)) for sc in scores]
            probs = [(ex / jnp.sum(ex, axis=-1, keepdims=True)).astype(BF16) for ex in exps]
            contexts = [jnp.dot(p, v, preferred_element_type=F32) for p, v in zip(probs, v_all)]
            for b, context in zip(group, contexts):
                for h in range(heads):
                    ctx[h, pl.ds(b, steps, stride=SEQS), :] = context[h * steps:(h + 1) * steps]
        for h in range(heads):
            mid[:, h * e:(h + 1) * e] = ctx[h].astype(BF16)

    def piece_ff(i):
        layer, c = lax.div(i, n_chunks), lax.rem(i, n_chunks)
        tile = 1024

        def block(j, carry):
            cols = mult(j * tile, tile)
            pre = jnp.dot(hbuf[c], w1[:, pl.ds(mult(3 * width + cols, 256), tile)], preferred_element_type=F32)
            pre = pre + bin_[layer, :, pl.ds(cols, tile)]
            inner = 0.7978845608028654 * (pre + 0.044715 * (pre * pre * pre))
            mid[:, pl.ds(mult(width + cols, 256), tile)] = (pre * (0.5 * (1.0 + jnp.tanh(inner)))).astype(BF16)
            return carry

        lax.fori_loop(0, d_ff // tile, block, 0, unroll=True)

    def piece_out(i):
        layer, s = lax.div(i, n_chunks), lax.rem(i, 2)
        tile = 1024

        def block(j, carry):
            cols = pl.ds(mult(j * tile, tile), tile)
            part[s, :, cols] = jnp.dot(mid[...], w2[:, cols], preferred_element_type=F32).astype(BF16)
            return carry

        lax.fori_loop(0, d_model // tile, block, 0, unroll=True)
        copy_a(i).start()
        next_weights(i, 4, 6)

    def copy_a(u):
        s2, s4 = lax.rem(u, 2), lax.rem(u, 4)
        return remote(part.at[s2, pl.ds(mult((1 - core) * half, half), half)], arecv.at[s4], a_send.at[s2], a_recv.at[s4], mate)

    def copies_b1(u):
        c, s4 = lax.rem(u, n_chunks), lax.rem(u, 4)
        return [remote(pair.at[s4, pl.ds(block_of(chip_o), sub)], b1r.at[0, c], b1_send.at[0, c], b1_recv.at[0, c], left),
                remote(pair.at[s4, pl.ds(mult(block_of(chip_o) + sub, sub), sub)], b1r.at[1, c], b1_send.at[1, c],
                       b1_recv.at[1, c], right)]

    def copies_bd(u):
        c, s4 = lax.rem(u, n_chunks), lax.rem(u, 4)
        return [remote(pair.at[s4, pl.ds(mult(block_of(chip_l) + sub, sub), sub)], b2r.at[0, c, pl.ds(sub, sub)],
                       bd_send.at[0, c], bd_recv.at[0, c], left),
                remote(pair.at[s4, pl.ds(block_of(chip_r), sub)], b2r.at[1, c, pl.ds(0, sub)],
                       bd_send.at[1, c], bd_recv.at[1, c], right)]

    def copies_b2(u):
        c, s4 = lax.rem(u, n_chunks), lax.rem(u, 4)
        return [remote(pair.at[s4, pl.ds(block_of(chip_l), sub)], b2r.at[0, c, pl.ds(0, sub)],
                       b2_send.at[0, c], b2_recv.at[0, c], left),
                remote(pair.at[s4, pl.ds(mult(block_of(chip_r) + sub, sub), sub)], b2r.at[1, c, pl.ds(sub, sub)],
                       b2_send.at[1, c], b2_recv.at[1, c], right)]

    def same_rows(c, start, size, send, recv, dev):
        ref = hbuf.at[c, pl.ds(start, size)]
        return remote(ref, ref, send, recv, dev)

    def copies_g1(u):
        c = lax.rem(u, n_chunks)
        mine = rows_of(chip)
        other = mult(mine + sub, sub)
        return [same_rows(c, other, sub, g1_send.at[0, c], g1_recv.at[0, c], left),
                same_rows(c, mine, sub, g1_send.at[1, c], g1_recv.at[1, c], right),
                same_rows(c, mine, sub, gn_send.at[0, c], gn_recv.at[0, c], left),
                same_rows(c, other, sub, gn_send.at[1, c], gn_recv.at[1, c], right),
                same_rows(c, mine, own_rows, d_send.at[0, c], d_recv.at[0, c], mate)]

    def copies_g2(u):
        c = lax.rem(u, n_chunks)
        from_r, from_l = rows_of(chip_r), rows_of(chip_l)
        return [same_rows(c, mult(from_r + sub, sub), sub, g2_send.at[0, c], g2_recv.at[0, c], left),
                same_rows(c, from_l, sub, g2_send.at[1, c], g2_recv.at[1, c], right),
                same_rows(c, from_r, own_rows, d_send.at[1, c], d_recv.at[1, c], mate),
                same_rows(c, from_l, own_rows, d_send.at[2, c], d_recv.at[2, c], mate)]

    def copy_g3(u):
        c = lax.rem(u, n_chunks)
        return same_rows(c, rows_of(chip_o), own_rows, d_send.at[3, c], d_recv.at[3, c], mate)

    def stage_b1(u):
        s2, s4 = lax.rem(u, 2), lax.rem(u, 4)
        copy_a(u).wait()

        def add(start):
            src = pl.ds(mult(core * half + start, BLOCK), BLOCK)
            dst = pl.ds(mult(start, BLOCK), BLOCK)
            pair[s4, dst] = (part[s2, src].astype(F32) + arecv[s4, dst].astype(F32)).astype(BF16)

        for t in range(own_rows // BLOCK):
            add(block_of(chip_o) + t * BLOCK)
        for copy in copies_b1(u):
            copy.start()
        add(block_of(chip_l) + sub)
        add(block_of(chip_r))
        for copy in copies_bd(u):
            copy.start()
        add(block_of(chip_l))
        add(block_of(chip_r) + sub)
        for t in range(own_rows // BLOCK):
            add(block_of(chip) + t * BLOCK)

    def stage_b2(u):
        c, s4 = lax.rem(u, n_chunks), lax.rem(u, 4)
        first, second = copies_b1(u), copies_b2(u)
        first[0].wait_recv()
        dst = pl.ds(block_of(chip_l), sub)
        pair[s4, dst] = (pair[s4, dst].astype(F32) + b1r[0, c].astype(F32)).astype(BF16)
        second[0].start()
        first[1].wait_recv()
        dst = pl.ds(mult(block_of(chip_r) + sub, sub), sub)
        pair[s4, dst] = (pair[s4, dst].astype(F32) + b1r[1, c].astype(F32)).astype(BF16)
        second[1].start()

    def stage_b3(u):
        layer, c, s4 = lax.div(u, n_chunks), lax.rem(u, n_chunks), lax.rem(u, 4)
        for copy in copies_bd(u) + copies_b2(u):
            copy.wait_recv()
        for t in range(own_rows // BLOCK):
            src = pl.ds(mult(block_of(chip) + t * BLOCK, BLOCK), BLOCK)
            loc = pl.ds(t * BLOCK, BLOCK)
            hid = own[c, loc].astype(F32) + bout[layer]
            hid = hid + (pair[s4, src].astype(F32) + (b2r[0, c, loc].astype(F32) + b2r[1, c, loc].astype(F32)))
            hid = hid.astype(BF16)
            dst = pl.ds(mult(rows_of(chip) + t * BLOCK, BLOCK), BLOCK)

            @pl.when(layer + 1 < n_layers)
            def _():
                own[c, loc] = hid
                nxt = layer + 1
                hbuf[c, dst] = normalise(hid.astype(F32), gain[nxt], bias[nxt]).astype(BF16)

            @pl.when(layer + 1 >= n_layers)
            def _():
                hbuf[c, dst] = hid

        for copy in copies_g1(u):
            copy.start()

    def stage_g2(u):
        second = copies_g2(u)
        c = lax.rem(u, n_chunks)
        from_r, from_l = rows_of(chip_r), rows_of(chip_l)
        same_rows(c, mult(from_r + sub, sub), sub, g1_send.at[0, c], g1_recv.at[0, c], left).wait_recv()
        second[0].start()
        same_rows(c, from_l, sub, g1_send.at[1, c], g1_recv.at[1, c], right).wait_recv()
        second[1].start()
        same_rows(c, from_r, sub, gn_send.at[0, c], gn_recv.at[0, c], left).wait_recv()
        second[2].start()
        same_rows(c, mult(from_l + sub, sub), sub, gn_send.at[1, c], gn_recv.at[1, c], right).wait_recv()
        second[3].start()

    def stage_g3(u):
        c = lax.rem(u, n_chunks)
        theirs = rows_of(chip_o)
        same_rows(c, mult(theirs + sub, sub), sub, g2_send.at[0, c], g2_recv.at[0, c], left).wait_recv()
        same_rows(c, theirs, sub, g2_send.at[1, c], g2_recv.at[1, c], right).wait_recv()
        copy_g3(u).start()
        for copy in copies_b1(u) + copies_bd(u) + copies_b2(u):
            copy.wait_send()

    def stage_g4(u):
        c = lax.rem(u, n_chunks)
        for n, q in enumerate((chip, chip_r, chip_l, chip_o)):
            start = mult((1 - core) * half + q * own_rows, own_rows)
            same_rows(c, start, own_rows, d_send.at[n, c], d_recv.at[n, c], mate).wait_recv()
        for copy in copies_g1(u) + copies_g2(u) + [copy_g3(u)]:
            copy.wait_send()

    def guarded(stage, u):
        @pl.when((u >= 0) & (u < total))
        def _():
            stage(u)

    parts = {"qkv": piece_qkv, "mid": piece_mid, "att": piece_attend, "out": piece_out, "b1": stage_b1, "b2": stage_b2, "b3": stage_b3,
             "g2": stage_g2, "g3": stage_g3, "g4": stage_g4}

    def greet():
        pl.semaphore_wait(barrier, 3)

    def fetch():
        own_copy.wait()
        for c in range(n_chunks):
            own[c] = xown[:, c * SEQS:(c + 1) * SEQS].astype(F32).reshape(own_rows, d_model).astype(BF16)

    def tick(i, carry):
        for name, lag in SCHEDULE:
            guarded(parts[name], i - lag)
            if name == "qkv":
                pl.when(i == 0)(greet)
            if name == "mid":
                pl.when(i == 1)(fetch)
        return carry

    lax.fori_loop(0, total + max(lag for _, lag in SCHEDULE), tick, 0)


def deliver(hid, k_new, v_new, hid_out, k_out, v_out, out_sem):
    n_chunks, rows, d_model = hid.shape
    steps = hid_out.shape[0]
    seqs = rows // steps
    moves = [(hid.at[c].reshape(steps, seqs, d_model), hid_out.at[:, pl.ds(c * seqs, seqs), :]) for c in range(n_chunks)]
    for src, dst in ((k_new, k_out), (v_new, v_out)):
        n_layers, batch = src.shape[:2]
        size = batch // 4
        moves += [(src.at[layer, pl.ds(b, size)], dst.at[layer, pl.ds(b, size)])
                  for layer in range(n_layers) for b in range(0, batch, size)]
    copies = [pltpu.make_async_copy(src, dst, out_sem.at[n]) for n, (src, dst) in enumerate(moves)]
    for copy in copies:
        copy.start()
    for copy in copies:
        copy.wait()


def decode_shard(x_steps, cur_len, k_cache, v_cache, ln_gain, ln_bias, w_q, w_k, w_v, w_o, w_in, b_in, w_out, b_out):
    steps, batch, d_model = x_steps.shape
    n_layers, _, slots, heads, head_dim = k_cache.shape
    d_ff = w_in.shape[2]
    n_chunks = batch // SEQS
    rows = steps * SEQS
    width = heads * head_dim
    own_rows = rows // 8
    tab = rotary_table(128, head_dim)
    k_rows = k_cache.reshape(n_layers, batch, slots * heads, head_dim)
    v_rows = v_cache.reshape(n_layers, batch, slots * heads, head_dim)
    vmem = pl.BlockSpec(memory_space=pltpu.VMEM)
    hbm = pl.BlockSpec(memory_space=pl.ANY)
    dims = (n_layers, n_chunks, steps, heads, head_dim, d_model, d_ff)
    dma = pltpu.SemaphoreType.DMA
    hid, k_new, v_new = pl.pallas_call(
        functools.partial(kernel, dims),
        out_shape=(pltpu.VMEM((n_chunks, rows, d_model), BF16), pltpu.VMEM(k_rows.shape, BF16), pltpu.VMEM(v_rows.shape, BF16)),
        in_specs=[pl.BlockSpec(memory_space=pltpu.SMEM)] + [vmem] * 5 + [hbm] * 9,
        out_specs=(vmem, vmem, vmem),
        scratch_shapes=[
            pltpu.VMEM((n_layers, 1, d_model), F32),
            pltpu.VMEM((n_layers, 1, d_model), F32),
            pltpu.VMEM((n_layers, 1, d_model), F32),
            pltpu.VMEM((n_layers, 1, d_ff), F32),
            pltpu.VMEM((d_model, 3 * width + d_ff), BF16),
            pltpu.VMEM((width + d_ff, d_model), BF16),
            pltpu.VMEM((n_chunks, own_rows, d_model), BF16),
            pltpu.VMEM((own_rows // SEQS, batch, d_model), BF16),
            pltpu.VMEM((2, steps, SEQS, d_model), BF16),
            pltpu.VMEM((2, SEQS, slots * heads, head_dim), BF16),
            pltpu.VMEM((2, SEQS, slots * heads, head_dim), BF16),
            pltpu.VMEM((3 * heads, rows, head_dim), F32),
            pltpu.VMEM((rows, 2 * head_dim), F32),
            pltpu.VMEM((heads, rows, head_dim), F32),
            pltpu.VMEM((rows, width + d_ff), BF16),
            pltpu.VMEM((2, rows, d_model), BF16),
            pltpu.VMEM((4, rows // 2, d_model), BF16),
            pltpu.VMEM((4, rows // 2, d_model), BF16),
            pltpu.VMEM((2, n_chunks, own_rows // 2, d_model), BF16),
            pltpu.VMEM((2, n_chunks, own_rows, d_model), BF16),
            dma((6,)), dma((2,)), dma, dma((2, 2)),
            dma((2,)), dma((4,)), dma((2, n_chunks)), dma((2, n_chunks)), dma((2, n_chunks)), dma((2, n_chunks)),
            dma((2, n_chunks)), dma((2, n_chunks)), dma((2, n_chunks)), dma((2, n_chunks)),
            dma((4, n_chunks)), dma((4, n_chunks)),
            dma((2, n_chunks)), dma((2, n_chunks)), dma((2, n_chunks)), dma((2, n_chunks)),
        ],
        compiler_params=pltpu.CompilerParams(collective_id=0, has_side_effects=True, vmem_limit_bytes=38 * 2**20),
    )(cur_len, tab, ln_gain, ln_bias, b_out, b_in, x_steps, k_rows, v_rows,
      w_q, w_k, w_v, w_in, w_o, w_out)
    hidden, k_new, v_new = pl.pallas_call(
        deliver,
        out_shape=(jax.ShapeDtypeStruct(x_steps.shape, BF16),
                   jax.ShapeDtypeStruct(k_rows.shape, BF16), jax.ShapeDtypeStruct(v_rows.shape, BF16)),
        in_specs=[vmem] * 3,
        out_specs=(hbm, hbm, hbm),
        scratch_shapes=[dma((n_chunks + 8 * n_layers,))],
        compiler_params=pltpu.CompilerParams(vmem_limit_bytes=2**20),
    )(*[pltpu.with_memory_space_constraint(a, pltpu.VMEM) for a in (hid, k_new, v_new)])
    return hidden, k_new.reshape(k_cache.shape), v_new.reshape(v_cache.shape)


def solution(mesh):
    cache_spec = P(None, "dp", None, "tp", None)
    in_specs = (P(None, "dp", None), P("dp"), cache_spec, cache_spec, P(None, None), P(None, None),
                P(None, None, "tp"), P(None, None, "tp"), P(None, None, "tp"), P(None, "tp", None),
                P(None, None, "tp"), P(None, "tp"), P(None, "tp", None), P(None, None))
    out_specs = (P(None, "dp", None), cache_spec, cache_spec)
    return jax.shard_map(decode_shard, mesh=mesh, in_specs=in_specs, out_specs=out_specs, check_vma=False)
```
